32 devices in a mesh: dp: 8 (over y, x, core), fsdp: 4 (over z).
Axes of the slice: x: 2, y: 2, z: 4, core: 2. Of those that a mesh axis runs over, the one named last changes fastest.
Arguments:
- hidden: bfloat16 [16384, 8192], P('dp', 'fsdp'), may hold values from -50 to 50
- logit_grad: bfloat16 [16384, 256], P('dp'), may hold values from -20 to 20
- master: float32 [256, 8192], P('dp', 'fsdp'), may hold values from -6 to 6
- moment_one: float32 [256, 8192], P('dp', 'fsdp'), may hold values from -4 to 4
- moment_two: float32 [256, 8192], P('dp', 'fsdp'), may hold values from 0.25 to 4
Outputs:
- new_rows: bfloat16 [256, 8192], P(None, 'fsdp')
- new_master: float32 [256, 8192], P('dp', 'fsdp')
- new_one: float32 [256, 8192], P('dp', 'fsdp')
- new_two: float32 [256, 8192], P('dp', 'fsdp')
The draws below stay inside these ranges and needn't reach their ends.
All inputs are finite; a program needn't handle non-finite values.
Results may differ from the reference program's by a relative error of at most 0.012.
Values may be sent and summed in bfloat16 or wider, within the bound.
A program may use at most 64 MiB of HBM per device.

```python
import math
import jax
import jax.numpy as jnp
from jax import lax

D = 8192
ROW_DEV = 32
TOK_DEV = 2048
ROWS = 256
TOKENS = 16384


def token_sign(key):
    flips = jax.random.bernoulli(jax.random.fold_in(key, 41), 0.5, (TOKENS,))
    return jnp.where(flips, 1.0, -1.0).astype(jnp.float32)


def draw_hidden(key, part):
    key_col = jax.random.fold_in(key, 11)
    key_val = jax.random.fold_in(key, 12)
    key_dir = jax.random.fold_in(key, 14)
    column = jnp.arange(D, dtype=jnp.float32) / D
    colscale = 10.0 ** jax.random.uniform(key_col, (D,), jnp.float32)
    colscale = colscale * 3.0 ** column
    sign = token_sign(key)
    direction = jax.random.truncated_normal(key_dir, -2.0, 2.0, (D,), jnp.float32)
    values = jax.random.truncated_normal(key_val, -4.0, 4.0, (TOKENS, D), jnp.float32)
    amount = 0.69 * float(TOK_DEV) ** (-0.25)
    values = values + amount * sign[:, None] * direction[None, :]
    scaled = values * colscale[None, :] / 3.0
    return jnp.clip(scaled, -50.0, 50.0).astype(jnp.bfloat16)


def draw_logit_grad(key, part):
    key_row = jax.random.fold_in(key, 21)
    key_val = jax.random.fold_in(key, 22)
    key_dir = jax.random.fold_in(key, 25)
    key_cell = jax.random.fold_in(key, 26)
    blocks = TOKENS // TOK_DEV
    row_blocks = ROWS // ROW_DEV
    position = jnp.arange(ROWS, dtype=jnp.float32) / ROWS
    spread = 10.0 ** jax.random.uniform(key_row, (ROWS,), jnp.float32)
    values = jax.random.truncated_normal(key_val, -4.0, 4.0, (TOKENS, ROWS), jnp.float32)
    sign = token_sign(key)
    direction = jax.random.truncated_normal(key_dir, -2.0, 2.0, (ROWS,), jnp.float32)
    rising = 3.0 ** position
    amount = 0.69 * float(TOK_DEV) ** (-0.25)
    values = values + amount * sign[:, None] * direction[None, :]
    values = 0.006 * values * (rising * spread)[None, :]
    cell = 10.0 ** jax.random.uniform(key_cell, (blocks, row_blocks), jnp.float32, -1.0, 1.0)
    values = values.reshape(blocks, TOK_DEV, row_blocks, ROW_DEV) * cell[:, None, :, None]
    values = values.reshape(TOKENS, ROWS)
    return jnp.clip(values, -20.0, 20.0).astype(jnp.bfloat16)


def block_levels(key, extent, pieces, smallest, high):
    loudness, own = 1.0, jax.random.fold_in(key, 6)
    for dim, blocks in pieces:
        steps = jnp.exp(jax.random.uniform(jax.random.fold_in(own, dim), (blocks,), jnp.float32, smallest / len(pieces), high / len(pieces)))
        loudness = loudness * jnp.repeat(steps, extent[dim] // blocks).reshape([-1 if axis == dim else 1 for axis in range(len(extent))])
    return loudness


def noise(stream_key, dims, scale, bound, split=(), kind=jnp.bfloat16):
    values = jax.random.normal(stream_key, dims, jnp.float32) * scale
    if len(split) > 0:
        values = block_levels(stream_key, dims, split, -0.22, 0.18) * values
    return jnp.clip(values, min=-bound, max=bound).astype(kind)


def setup_inputs(seed: int = 0) -> dict:
    streams_of = jax.random.split(jax.random.key(seed), 6)
    hidden = draw_hidden(jax.random.fold_in(streams_of[5], 71), 0)
    logit_grad = draw_logit_grad(jax.random.fold_in(streams_of[5], 71), 0)
    master = noise(streams_of[2], (ROWS, D), 1.0, 6.0, ((0, 8), (1, 4)), jnp.float32)
    moment_one = noise(streams_of[3], (ROWS, D), 0.5, 4.0, ((0, 8), (1, 4)), jnp.float32)
    moment_two = jnp.clip(jnp.exp(math.log(4.0) - 2.7725887 * jax.random.uniform(streams_of[4], (ROWS, D), jnp.float32) ** block_levels(streams_of[4], (ROWS, D), ((0, 8), (1, 4)), -0.2, 0.2)), 0.25, 4.0)
    return dict(hidden=hidden, logit_grad=logit_grad, master=master, moment_one=moment_one, moment_two=moment_two)


def reference(hidden, logit_grad, master, moment_one, moment_two):
    blocks = TOKENS // TOK_DEV
    hid = hidden.reshape(blocks, TOK_DEV, D)
    lgr = logit_grad.reshape(blocks, TOK_DEV, ROWS)

    def accumulate(total, pair):
        states, grads = pair
        part = lax.dot_general(grads, states, (((0,), (0,)), ((), ())), preferred_element_type=jnp.float32)
        part = lax.optimization_barrier(part.astype(jnp.bfloat16)).astype(jnp.float32)
        return (total + part, None)
    grad, _ = lax.scan(accumulate, jnp.zeros((ROWS, D), jnp.float32), (hid, lgr))
    sumsq = jnp.sum(grad * grad)
    rms = jnp.sqrt(sumsq / (ROWS * D))
    factor = jnp.minimum(1.0, 1.0 / rms)
    clipped = factor * grad
    new_one = 0.9 * moment_one + 0.1 * clipped
    new_two = 0.95 * moment_two + 0.05 * clipped * clipped
    first = new_one / (1.0 - 0.9 ** 10)
    second = new_two / (1.0 - 0.95 ** 10)
    new_master = master - 0.05 * (first / (jnp.sqrt(second) + 1e-08) + 0.1 * master)
    return (new_master.astype(jnp.bfloat16), new_master, new_one, new_two)
```

```python
import functools

import jax
import jax.numpy as jnp
from jax import lax
from jax.experimental import pallas as pl
from jax.experimental.pallas import tpu as pltpu
from jax.sharding import PartitionSpec as P

MESH = pl.DeviceIdType.MESH
LOAD_CHUNKS = 4
GATHER_CHUNKS = 2
VMEM_BYTES = 67_043_328
UNITS = 8
PARTS = 4
CHUNKS = ((1, False), (2, False), (2, False), (2, False), (1, False))
PIECES = ((2, True), (2, False), (2, False), (2, False))
AHEAD = 2


def pieces(width, wanted):
    count = wanted
    while count > 1 and width % (count * 128):
        count -= 1
    return count


def direct_kernel(
    n, depth, chunks, gathers,
    hid, lgr, mas, one, two,
    rows_out, mas_out, one_out, two_out,
    lgr_v, lgt_v, hid_v, mas_v, one_v, two_v,
    stage, paired, sums, arrived, grad, sq_all,
    hid_sem, lgr_sem, state_sem, pair_send, pair_recv, chip_send, chip_recv,
    sq_send, sq_recv, ag_send, ag_recv, relay_send, relay_recv,
):
    chips = n // 2
    total = n * depth
    rows, width = grad.shape
    dp, fs = lax.axis_index("dp"), lax.axis_index("fsdp")
    chip, core = dp // 2, dp % 2
    other = 1 - core
    me = dp * depth + fs
    wc, wa = width // chunks, width // gathers

    lgr_copy = pltpu.make_async_copy(lgr, lgr_v, lgr_sem)
    lgr_copy.start()
    loads = []
    for j in range(chunks):
        load = pltpu.make_async_copy(hid.at[:, pl.ds(j * wc, wc)], hid_v.at[j], hid_sem.at[j])
        load.start()
        loads.append(load)
    states = []
    for i, (src, dst) in enumerate(((mas, mas_v), (one, one_v), (two, two_v))):
        load = pltpu.make_async_copy(src, dst, state_sem.at[i])
        load.start()
        states.append(load)

    def each_other_device(act):
        def visit(i):
            index = (me + i) % total
            act((index // depth, index % depth))

        if total <= 64:
            for i in range(1, total):
                visit(i)
        else:
            lax.fori_loop(1, total, lambda i, carry: (visit(i), carry)[1], 0)

    barrier = pltpu.get_barrier_semaphore()
    each_other_device(
        lambda to: pl.semaphore_signal(barrier, inc=1, device_id=to, device_id_type=MESH)
    )

    lgr_copy.wait()
    lgt_v[...] = lgr_v[...].T

    def remote(src, dst, send, recv, to):
        return pltpu.make_async_remote_copy(
            src_ref=src, dst_ref=dst, send_sem=send, recv_sem=recv, device_id=to, device_id_type=MESH
        )

    partner = (2 * chip + other, fs)
    others = [(chip + o) % chips for o in range(1, chips)]

    def pair_copy(j):
        return remote(stage.at[j, other], paired.at[j], pair_send.at[j], pair_recv.at[j], partner)

    def chip_copy(j, q, slot):
        return remote(
            sums.at[j, q], arrived.at[j, slot], chip_send.at[j, q], chip_recv.at[j, slot],
            (2 * q + core, fs),
        )

    def chip_sum(j):
        pair_copy(j).wait_recv()
        for q in others:
            both = stage[j, core, q].astype(jnp.float32) + paired[j, q].astype(jnp.float32)
            sums[j, q] = both.astype(jnp.bfloat16)
            chip_copy(j, q, chip).start()
        grad[:, pl.ds(j * wc, wc)] = stage[j, core, chip].astype(jnp.float32) + paired[
            j, chip
        ].astype(jnp.float32)

    for j in range(chunks):
        loads[j].wait()
        part = jnp.dot(lgt_v[...], hid_v[j], preferred_element_type=jnp.float32)
        part = part.astype(jnp.bfloat16)
        for q in range(chips):
            for c in range(2):
                d = 2 * q + c
                stage[j, c, q] = part[d * rows : (d + 1) * rows, :]
        if j == 0:
            pl.semaphore_wait(barrier, total - 1)
        pair_copy(j).start()
        if j > 0:
            chip_sum(j - 1)
    chip_sum(chunks - 1)

    squares = jnp.zeros((1, 128), jnp.float32)
    for j in range(chunks):
        span = pl.ds(j * wc, wc)
        value = grad[:, span]
        for q in others:
            chip_copy(j, q, q).wait_recv()
            value = value + arrived[j, q].astype(jnp.float32)
        grad[:, span] = value
        column = jnp.sum(value * value, axis=0, keepdims=True)
        for s in range(wc // 128):
            squares = squares + column[:, s * 128 : (s + 1) * 128]

    sq_all[me] = squares
    each_other_device(
        lambda to: remote(sq_all.at[me], sq_all.at[me], sq_send, sq_recv, to).start()
    )
    for load in states:
        load.wait()
    everyone = sq_all.at[pl.ds(0, total - 1)]
    pltpu.make_async_copy(everyone, everyone, sq_recv).wait()
    sumsq = jnp.sum(jnp.sum(sq_all[...], axis=0), axis=1, keepdims=True)
    rms = jnp.sqrt(sumsq / (rows * n * width * depth))
    factor = jnp.where(rms > 1.0, 1.0 / rms, 1.0)

    def cols(k):
        return pl.ds(k * wa, wa)

    def rows_of(d):
        return pl.ds(pl.multiple_of(d * rows, rows), rows)

    def gather_copy(k, d, to, send, recv):
        block = rows_out.at[rows_of(d), cols(k)]
        return remote(block, block, send, recv, to)

    def direct(k, source, q):
        return gather_copy(k, 2 * source + core, (2 * q + core, fs), ag_send.at[k, q], ag_recv.at[k, source])

    def relay(k, q, side):
        return gather_copy(k, 2 * q + side, partner, relay_send.at[k, q], relay_recv.at[k, q])

    for k in range(gathers):
        span = cols(k)
        clipped = factor * grad[:, span]
        new_one = 0.9 * one_v[:, span] + 0.1 * clipped
        new_two = 0.95 * two_v[:, span] + 0.05 * clipped * clipped
        first = new_one / (1.0 - 0.9**10)
        second = new_two / (1.0 - 0.95**10)
        held = mas_v[:, span]
        new_master = held - 0.05 * (first / (jnp.sqrt(second) + 1e-08) + 0.1 * held)
        rows_out[rows_of(dp), span] = new_master.astype(jnp.bfloat16)
        for q in others:
            direct(k, chip, q).start()
        relay(k, chip, core).start()
        one_out[:, span] = new_one
        two_out[:, span] = new_two
        mas_out[:, span] = new_master
    for k in range(gathers):
        for q in others:
            direct(k, q, q).wait_recv()
            relay(k, q, core).start()
    for k in range(gathers):
        for q in [chip] + others:
            relay(k, q, other).wait_recv()

    for j in range(chunks):
        pair_copy(j).wait_send()
        for q in others:
            chip_copy(j, q, chip).wait_send()
    pltpu.make_async_copy(everyone, everyone, sq_send).wait()
    for k in range(gathers):
        for q in others:
            direct(k, chip, q).wait_send()
            relay(k, q, core).wait_send()
        relay(k, chip, core).wait_send()


def spans(width, plan):
    unit, start, result = width // UNITS, 0, []
    for count, relayed in plan:
        result.append((start, count * unit, relayed))
        start += count * unit
    return result


def square_scratch(n, depth, tokens, slab, rows, width):
    f32, bf16 = jnp.float32, jnp.bfloat16
    dma = pltpu.SemaphoreType.DMA
    chunks = [(w, relayed) for _, w, relayed in spans(width, CHUNKS)]
    state = pltpu.VMEM((rows, width), f32)
    stage = tuple(pltpu.VMEM((2, n // 2, rows, w), bf16) for w, _ in chunks)
    paired = tuple(pltpu.VMEM((n // 2, rows, w), bf16) for w, _ in chunks)
    first = tuple(
        pltpu.VMEM((2, 2, rows, w // 2) if relayed else (3, rows, w), bf16) for w, relayed in chunks
    )
    second = tuple(pltpu.VMEM((2, rows, w // 2), bf16) for w, _ in chunks)
    many = len(chunks)
    return [
        pltpu.VMEM((tokens, slab), bf16),
        pltpu.VMEM((slab, tokens), bf16),
        tuple(pltpu.VMEM((tokens, w), bf16) for w, _ in chunks),
        state, state, state, state,
        stage, paired, first, first, second, second,
        pltpu.VMEM((n * depth, 1, 128), f32),
        dma((PARTS,)), dma((many,)), dma((3,)),
        dma, dma((many,)),
        dma((many,)), dma((many, 3)),
        dma((many,)), dma((many, 2)),
        dma, dma,
        dma((2,)), dma((len(PIECES), 3)),
        dma, dma((len(PIECES), 2)),
        dma, dma,
    ]


def square_kernel(
    n, depth,
    hid, lgr, mas, one, two,
    rows_out, mas_out, one_out, two_out,
    lgr_v, lgt_v, hid_v, mas_v, one_v, two_v, grad,
    stage, paired, p1_out, p1_in, p2_out, p2_in, sq_all,
    lgr_sem, hid_sem, state_sem, pair_send, pair_recv, p1_send, p1_recv, p2_send, p2_recv,
    sq_send, sq_recv, ag_send, ag_recv, far_send, far_recv, relay_send, relay_recv,
):
    total = n * depth
    rows, width = grad.shape
    f32, bf16 = jnp.float32, jnp.bfloat16
    dp, fs = lax.axis_index("dp"), lax.axis_index("fsdp")
    chip, core = dp // 2, dp % 2
    other = 1 - core
    x, y = chip % 2, chip // 2
    near = (2 * y + 1 - x, 2 * (1 - y) + x)
    far = 2 * (1 - y) + 1 - x
    me = dp * depth + fs
    partner = (2 * chip + other, fs)
    across = tuple((2 * q + core, fs) for q in near + (far,))
    chunks, pieces_ = spans(width, CHUNKS), spans(width, PIECES)
    steps = sorted(
        ((z, b, a, c) for z in range(depth) for b in range(2) for a in range(2) for c in range(2)),
        key=lambda s: -(min(s[0], depth - s[0]) + s[1] + s[2] + s[3] / 4),
    )[:-1]

    def each_other_device(act):
        for dz, b, a, c in steps:
            to_y = 1 - y if b else y
            to_x = 1 - x if a else x
            to_core = other if c else core
            act(((2 * to_y + to_x) * 2 + to_core, (fs + dz) % depth))

    def remote(src, dst, send, recv, to):
        return pltpu.make_async_remote_copy(
            src_ref=src, dst_ref=dst, send_sem=send, recv_sem=recv, device_id=to, device_id_type=MESH
        )

    def settle(ref, sem):
        pltpu.make_async_copy(ref, ref, sem).wait()

    step = lgr.shape[0] // PARTS
    lgr_loads = [
        pltpu.make_async_copy(lgr.at[pl.ds(i * step, step)], lgr_v.at[pl.ds(i * step, step)], lgr_sem.at[i])
        for i in range(PARTS)
    ]
    for load in lgr_loads:
        load.start()
    loads = [
        pltpu.make_async_copy(hid.at[:, pl.ds(start, w)], hid_v[j], hid_sem.at[j])
        for j, (start, w, _) in enumerate(chunks)
    ]
    for load in loads[:AHEAD]:
        load.start(priority=1)
    barrier = pltpu.get_barrier_semaphore()
    each_other_device(
        lambda to: pl.semaphore_signal(barrier, inc=1, device_id=to, device_id_type=MESH)
    )
    states = [
        pltpu.make_async_copy(src, dst, state_sem.at[i])
        for i, (src, dst) in enumerate(((mas, mas_v), (one, one_v), (two, two_v)))
    ]

    def pair_copy(j):
        return remote(stage[j].at[other], paired[j], pair_send, pair_recv.at[j], partner)

    def first_copy(j, way):
        return remote(p1_out[j].at[way], p1_in[j].at[way], p1_send.at[j], p1_recv.at[j, way], across[way])

    def second_copy(j, way):
        return remote(p2_out[j].at[way], p2_in[j].at[way], p2_send.at[j], p2_recv.at[j, way], across[way])

    def both(j, q, start, w):
        cols = pl.ds(start, w)
        return stage[j][core, q, :, cols].astype(f32) + paired[j][q, :, cols].astype(f32)

    def chip_sum(j):
        start, w, relayed = chunks[j]
        wh = w // 2
        pair_copy(j).wait_recv()
        if relayed:
            for way in range(2):
                p1_out[j][way, 1] = both(j, far, way * wh, wh).astype(bf16)
                p1_out[j][way, 0] = both(j, near[way], way * wh, wh).astype(bf16)
                first_copy(j, way).start()
        else:
            for way, q in ((2, far), (0, near[0]), (1, near[1])):
                p1_out[j][way] = both(j, q, 0, w).astype(bf16)
                first_copy(j, way).start()
        grad[:, pl.ds(start, w)] = both(j, chip, 0, w)

    for i in range(PARTS):
        lgr_loads[i].wait()
        lgt_v[:, i * step : (i + 1) * step] = lgr_v[i * step : (i + 1) * step, :].T
    for j in range(len(chunks)):
        loads[j].wait()
        if j + AHEAD < len(chunks):
            loads[j + AHEAD].start(priority=1)
        part = jnp.dot(lgt_v[...], hid_v[j][...], preferred_element_type=f32).astype(bf16)
        for q in range(n // 2):
            for c in range(2):
                d = 2 * q + c
                stage[j][c, q] = part[d * rows : (d + 1) * rows, :]
        if j == 0:
            pl.semaphore_wait(barrier, total - 1)
        pair_copy(j).start()
        if j > 0:
            chip_sum(j - 1)
    for load in states:
        load.start()
    chip_sum(len(chunks) - 1)

    relayed_chunks = [j for j in range(len(chunks)) if chunks[j][2]]
    for j in relayed_chunks:
        wh = chunks[j][1] // 2
        for way in range(2):
            first_copy(j, way).wait_recv()
            away = 1 - way
            joined = both(j, near[away], way * wh, wh) + p1_in[j][way, 1].astype(f32)
            p2_out[j][away] = joined.astype(bf16)
            second_copy(j, away).start()

    squares = jnp.zeros((8, 128), f32)

    def add(start, w, terms, squares):
        span = pl.ds(start, w)
        value = grad[:, span]
        for term in terms:
            value = value + term.astype(f32)
        grad[:, span] = value
        value = value * value
        for r in range(rows // 8):
            for s in range(w // 128):
                squares = squares + value[r * 8 : (r + 1) * 8, s * 128 : (s + 1) * 128]
        return squares

    for j in relayed_chunks:
        start, w, _ = chunks[j]
        wh = w // 2
        for way in range(2):
            second_copy(j, 1 - way).wait_recv()
            squares = add(start + way * wh, wh, (p1_in[j][way, 0], p2_in[j][1 - way]), squares)
    for j, (start, w, relayed) in enumerate(chunks):
        if not relayed:
            for way in range(3):
                first_copy(j, way).wait_recv()
            squares = add(start, w, [p1_in[j][way] for way in range(3)], squares)

    sq_all[me] = jnp.sum(squares, axis=0, keepdims=True)
    each_other_device(
        lambda to: remote(sq_all.at[me], sq_all.at[me], sq_send, sq_recv, to).start()
    )
    for load in states:
        load.wait()
    everyone = sq_all.at[pl.ds(0, total - 1)]
    settle(everyone, sq_recv)
    sumsq = jnp.sum(jnp.sum(sq_all[...], axis=0), axis=1, keepdims=True)
    rms = jnp.sqrt(sumsq / (rows * n * width * depth))
    factor = jnp.where(rms > 1.0, 1.0 / rms, 1.0)

    def block(q, start, w):
        return rows_out.at[pl.ds(pl.multiple_of((2 * q + core) * rows, rows), rows), pl.ds(start, w)]

    def own_copy(k, way, q):
        start, w, relayed = pieces_[k]
        sem = ag_send.at[0 if relayed else 1]
        return remote(block(q, start, w), block(q, start, w), sem, ag_recv.at[k, way], across[way])

    def far_copy(k, way, q):
        start, w, _ = pieces_[k]
        part = block(q, start + way * (w // 2), w // 2)
        return remote(part, part, far_send, far_recv.at[k, way], across[1 - way])

    def relay(q, start, w):
        return remote(block(q, start, w), block(q, start, w), relay_send, relay_recv, partner)

    for k, (start, w, relayed) in enumerate(pieces_):
        span = pl.ds(start, w)
        clipped = factor * grad[:, span]
        new_one = 0.9 * one_v[:, span] + 0.1 * clipped
        new_two = 0.95 * two_v[:, span] + 0.05 * clipped * clipped
        first = new_one / (1.0 - 0.9**10)
        second = new_two / (1.0 - 0.95**10)
        held = mas_v[:, span]
        new_master = held - 0.05 * (first / (jnp.sqrt(second) + 1e-08) + 0.1 * held)
        rows_out[pl.ds(pl.multiple_of(dp * rows, rows), rows), span] = new_master.astype(bf16)
        for way in (0, 1) if relayed else (2, 0, 1):
            own_copy(k, way, chip).start()
        relay(chip, start, w).start()
        one_out[:, span] = new_one
        two_out[:, span] = new_two
        mas_out[:, span] = new_master

    for k, (start, w, relayed) in enumerate(pieces_):
        if relayed:
            for way in range(2):
                own_copy(k, way, near[way]).wait_recv()
                far_copy(k, way, near[way]).start()
                relay(near[way], start, w).start()
    for k, (start, w, relayed) in enumerate(pieces_):
        if not relayed:
            for way, q in ((0, near[0]), (1, near[1]), (2, far)):
                own_copy(k, way, q).wait_recv()
                relay(q, start, w).start()
    for k, (start, w, relayed) in enumerate(pieces_):
        if relayed:
            for way in range(2):
                far_copy(k, way, far).wait_recv()
                relay(far, start + way * (w // 2), w // 2).start()

    for j, (_, w, relayed) in enumerate(chunks):
        settle(paired[j], pair_send)
        settle(p1_in[j], p1_send.at[j])
        if relayed:
            settle(p2_in[j], p2_send.at[j])
    settle(everyone, sq_send)
    sent = sum(w for _, w, relayed in pieces_ if relayed)
    settle(rows_out.at[pl.ds(0, 2 * rows), pl.ds(0, sent)], ag_send.at[0])
    settle(rows_out.at[pl.ds(0, rows), pl.ds(0, sent)], far_send)
    if sent < width:
        settle(rows_out.at[pl.ds(0, 3 * rows), pl.ds(0, width - sent)], ag_send.at[1])
    settle(rows_out.at[pl.ds(0, 4 * rows)], relay_send)
    settle(rows_out.at[pl.ds(0, 4 * rows)], relay_recv)


def write_out(*refs):
    sems = refs[8]
    copies = [pltpu.make_async_copy(refs[i], refs[4 + i], sems.at[i]) for i in range(4)]
    for copy in copies:
        copy.start()
    for copy in copies:
        copy.wait()


def shards(n, depth, hidden, logit_grad, master, moment_one, moment_two):
    tokens, width = hidden.shape
    slab = logit_grad.shape[1]
    rows = master.shape[0]
    chips = n // 2
    f32, bf16 = jnp.float32, jnp.bfloat16
    state = ((rows, width), f32)
    shapes = (((slab, width), bf16), state, state, state)
    kept = slab * width * 2 + 3 * rows * width * 4
    dma = pltpu.SemaphoreType.DMA
    anywhere = pl.BlockSpec(memory_space=pl.ANY)
    in_vmem = pl.BlockSpec(memory_space=pltpu.VMEM)
    if n == 8 and width % (UNITS * 256) == 0 and tokens % (PARTS * 128) == 0:
        body = functools.partial(square_kernel, n, depth)
        scratch = square_scratch(n, depth, tokens, slab, rows, width)
    else:
        chunks = pieces(width, LOAD_CHUNKS)
        gathers = pieces(width, GATHER_CHUNKS)
        wc = width // chunks
        body = functools.partial(direct_kernel, n, depth, chunks, gathers)
        scratch = [
            pltpu.VMEM((tokens, slab), bf16),
            pltpu.VMEM((slab, tokens), bf16),
            pltpu.VMEM((chunks, tokens, wc), bf16),
            pltpu.VMEM((rows, width), f32),
            pltpu.VMEM((rows, width), f32),
            pltpu.VMEM((rows, width), f32),
            pltpu.VMEM((chunks, 2, chips, rows, wc), bf16),
            pltpu.VMEM((chunks, chips, rows, wc), bf16),
            pltpu.VMEM((chunks, chips, rows, wc), bf16),
            pltpu.VMEM((chunks, chips, rows, wc), bf16),
            pltpu.VMEM((rows, width), f32),
            pltpu.VMEM((n * depth, 1, 128), f32),
            dma((chunks,)),
            dma,
            dma((3,)),
            dma((chunks,)),
            dma((chunks,)),
            dma((chunks, chips)),
            dma((chunks, chips)),
            dma,
            dma,
            dma((gathers, chips)),
            dma((gathers, chips)),
            dma((gathers, chips)),
            dma((gathers, chips)),
        ]
    held = pl.pallas_call(
        body,
        out_shape=tuple(pltpu.VMEM(*shape) for shape in shapes),
        in_specs=[anywhere] * 5,
        out_specs=(in_vmem,) * 4,
        scratch_shapes=scratch,
        compiler_params=pltpu.CompilerParams(
            collective_id=0, has_side_effects=True, vmem_limit_bytes=VMEM_BYTES - kept - 96 * 1024
        ),
    )(hidden, logit_grad, master, moment_one, moment_two)
    return pl.pallas_call(
        write_out,
        out_shape=tuple(pltpu.HBM(*shape) for shape in shapes),
        in_specs=[anywhere] * 4,
        out_specs=(anywhere,) * 4,
        scratch_shapes=[dma((4,))],
        compiler_params=pltpu.CompilerParams(vmem_limit_bytes=1024 * 1024),
    )(*held)


def solution(mesh):
    placed = (P("dp", "fsdp"), P("dp", None), P("dp", "fsdp"), P("dp", "fsdp"), P("dp", "fsdp"))
    return jax.shard_map(
        functools.partial(shards, mesh.shape["dp"], mesh.shape["fsdp"]),
        mesh=mesh,
        in_specs=placed,
        out_specs=(P(None, "fsdp"), P("dp", "fsdp"), P("dp", "fsdp"), P("dp", "fsdp")),
        check_vma=False,
    )
```

```python
import functools

import jax
import jax.numpy as jnp
from jax import lax
from jax.experimental import pallas as pl
from jax.experimental.pallas import tpu as pltpu
from jax.sharding import PartitionSpec as P

MESH = pl.DeviceIdType.MESH
LOAD_CHUNKS = 4
GATHER_CHUNKS = 2
VMEM_BYTES = 67_043_328
UNITS = 8
PARTS = 4
CHUNKS = ((1, False), (2, False), (2, False), (3, False))
PIECES = ((2, True), (2, False), (3, False))
KITS = 1
EARLY = 0
AHEAD = 2


def pieces(width, wanted):
    count = wanted
    while count > 1 and width % (count * 128):
        count -= 1
    return count


def direct_kernel(
    n, depth, chunks, gathers,
    hid, lgr, mas, one, two,
    rows_out, mas_out, one_out, two_out,
    lgr_v, lgt_v, hid_v, mas_v, one_v, two_v,
    stage, paired, sums, arrived, grad, sq_all,
    hid_sem, lgr_sem, state_sem, pair_send, pair_recv, chip_send, chip_recv,
    sq_send, sq_recv, ag_send, ag_recv, relay_send, relay_recv,
):
    chips = n // 2
    total = n * depth
    rows, width = grad.shape
    dp, fs = lax.axis_index("dp"), lax.axis_index("fsdp")
    chip, core = dp // 2, dp % 2
    other = 1 - core
    me = dp * depth + fs
    wc, wa = width // chunks, width // gathers

    lgr_copy = pltpu.make_async_copy(lgr, lgr_v, lgr_sem)
    lgr_copy.start()
    loads = []
    for j in range(chunks):
        load = pltpu.make_async_copy(hid.at[:, pl.ds(j * wc, wc)], hid_v.at[j], hid_sem.at[j])
        load.start()
        loads.append(load)
    states = []
    for i, (src, dst) in enumerate(((mas, mas_v), (one, one_v), (two, two_v))):
        load = pltpu.make_async_copy(src, dst, state_sem.at[i])
        load.start()
        states.append(load)

    def each_other_device(act):
        def visit(i):
            index = (me + i) % total
            act((index // depth, index % depth))

        if total <= 64:
            for i in range(1, total):
                visit(i)
        else:
            lax.fori_loop(1, total, lambda i, carry: (visit(i), carry)[1], 0)

    barrier = pltpu.get_barrier_semaphore()
    each_other_device(
        lambda to: pl.semaphore_signal(barrier, inc=1, device_id=to, device_id_type=MESH)
    )

    lgr_copy.wait()
    lgt_v[...] = lgr_v[...].T

    def remote(src, dst, send, recv, to):
        return pltpu.make_async_remote_copy(
            src_ref=src, dst_ref=dst, send_sem=send, recv_sem=recv, device_id=to, device_id_type=MESH
        )

    partner = (2 * chip + other, fs)
    others = [(chip + o) % chips for o in range(1, chips)]

    def pair_copy(j):
        return remote(stage.at[j, other], paired.at[j], pair_send.at[j], pair_recv.at[j], partner)

    def chip_copy(j, q, slot):
        return remote(
            sums.at[j, q], arrived.at[j, slot], chip_send.at[j, q], chip_recv.at[j, slot],
            (2 * q + core, fs),
        )

    def chip_sum(j):
        pair_copy(j).wait_recv()
        for q in others:
            both = stage[j, core, q].astype(jnp.float32) + paired[j, q].astype(jnp.float32)
            sums[j, q] = both.astype(jnp.bfloat16)
            chip_copy(j, q, chip).start()
        grad[:, pl.ds(j * wc, wc)] = stage[j, core, chip].astype(jnp.float32) + paired[
            j, chip
        ].astype(jnp.float32)

    for j in range(chunks):
        loads[j].wait()
        part = jnp.dot(lgt_v[...], hid_v[j], preferred_element_type=jnp.float32)
        part = part.astype(jnp.bfloat16)
        for q in range(chips):
            for c in range(2):
                d = 2 * q + c
                stage[j, c, q] = part[d * rows : (d + 1) * rows, :]
        if j == 0:
            pl.semaphore_wait(barrier, total - 1)
        pair_copy(j).start()
        if j > 0:
            chip_sum(j - 1)
    chip_sum(chunks - 1)

    squares = jnp.zeros((1, 128), jnp.float32)
    for j in range(chunks):
        span = pl.ds(j * wc, wc)
        value = grad[:, span]
        for q in others:
            chip_copy(j, q, q).wait_recv()
            value = value + arrived[j, q].astype(jnp.float32)
        grad[:, span] = value
        column = jnp.sum(value * value, axis=0, keepdims=True)
        for s in range(wc // 128):
            squares = squares + column[:, s * 128 : (s + 1) * 128]

    sq_all[me] = squares
    each_other_device(
        lambda to: remote(sq_all.at[me], sq_all.at[me], sq_send, sq_recv, to).start()
    )
    for load in states:
        load.wait()
    everyone = sq_all.at[pl.ds(0, total - 1)]
    pltpu.make_async_copy(everyone, everyone, sq_recv).wait()
    sumsq = jnp.sum(jnp.sum(sq_all[...], axis=0), axis=1, keepdims=True)
    rms = jnp.sqrt(sumsq / (rows * n * width * depth))
    factor = jnp.where(rms > 1.0, 1.0 / rms, 1.0)

    def cols(k):
        return pl.ds(k * wa, wa)

    def rows_of(d):
        return pl.ds(pl.multiple_of(d * rows, rows), rows)

    def gather_copy(k, d, to, send, recv):
        block = rows_out.at[rows_of(d), cols(k)]
        return remote(block, block, send, recv, to)

    def direct(k, source, q):
        return gather_copy(k, 2 * source + core, (2 * q + core, fs), ag_send.at[k, q], ag_recv.at[k, source])

    def relay(k, q, side):
        return gather_copy(k, 2 * q + side, partner, relay_send.at[k, q], relay_recv.at[k, q])

    for k in range(gathers):
        span = cols(k)
        clipped = factor * grad[:, span]
        new_one = 0.9 * one_v[:, span] + 0.1 * clipped
        new_two = 0.95 * two_v[:, span] + 0.05 * clipped * clipped
        first = new_one / (1.0 - 0.9**10)
        second = new_two / (1.0 - 0.95**10)
        held = mas_v[:, span]
        new_master = held - 0.05 * (first / (jnp.sqrt(second) + 1e-08) + 0.1 * held)
        rows_out[rows_of(dp), span] = new_master.astype(jnp.bfloat16)
        for q in others:
            direct(k, chip, q).start()
        relay(k, chip, core).start()
        one_out[:, span] = new_one
        two_out[:, span] = new_two
        mas_out[:, span] = new_master
    for k in range(gathers):
        for q in others:
            direct(k, q, q).wait_recv()
            relay(k, q, core).start()
    for k in range(gathers):
        for q in [chip] + others:
            relay(k, q, other).wait_recv()

    for j in range(chunks):
        pair_copy(j).wait_send()
        for q in others:
            chip_copy(j, q, chip).wait_send()
    pltpu.make_async_copy(everyone, everyone, sq_send).wait()
    for k in range(gathers):
        for q in others:
            direct(k, chip, q).wait_send()
            relay(k, q, core).wait_send()
        relay(k, chip, core).wait_send()


def spans(width, plan):
    unit, start, result = width // UNITS, 0, []
    for count, relayed in plan:
        result.append((start, count * unit, relayed))
        start += count * unit
    return result


def square_scratch(n, depth, tokens, slab, rows, width):
    f32, bf16 = jnp.float32, jnp.bfloat16
    dma = pltpu.SemaphoreType.DMA
    chunks = [(w, relayed) for _, w, relayed in spans(width, CHUNKS)]
    state = pltpu.VMEM((rows, width), f32)
    stage = tuple(pltpu.VMEM((2, n // 2, rows, w), bf16) for w, _ in chunks)
    paired = tuple(pltpu.VMEM((n // 2, rows, w), bf16) for w, _ in chunks)
    first = tuple(
        pltpu.VMEM((2, 2, rows, w // 2) if relayed else (3, rows, w), bf16) for w, relayed in chunks
    )
    second = tuple(pltpu.VMEM((2, rows, w // 2), bf16) for w, _ in chunks)
    many = len(chunks)
    return [
        pltpu.VMEM((tokens, slab), bf16),
        pltpu.VMEM((slab, tokens), bf16),
        tuple(pltpu.VMEM((tokens, w), bf16) for w, _ in chunks),
        state, state, state, state,
        stage, paired, first, first, second, second,
        tuple(pltpu.VMEM((4, 4, rows, width // UNITS), bf16) for _ in range(KITS)),
        pltpu.VMEM((n * depth, 1, 128), f32),
        dma((PARTS,)), dma((many,)), dma((3,)),
        dma, dma((many,)),
        dma((many,)), dma((many, 3)),
        dma((many,)), dma((many, 2)),
        dma, dma,
        dma((2,)), dma((len(PIECES), 3)),
        dma, dma((len(PIECES), 2)),
        dma, dma,
        dma((KITS,)), dma((KITS, 2, 3)),
    ]


def square_kernel(
    n, depth,
    hid, lgr, mas, one, two,
    rows_out, mas_out, one_out, two_out,
    lgr_v, lgt_v, hid_v, mas_v, one_v, two_v, grad,
    stage, paired, p1_out, p1_in, p2_out, p2_in, kit, sq_all,
    lgr_sem, hid_sem, state_sem, pair_send, pair_recv, p1_send, p1_recv, p2_send, p2_recv,
    sq_send, sq_recv, ag_send, ag_recv, far_send, far_recv, relay_send, relay_recv,
    kit_send, kit_recv,
):
    total = n * depth
    rows, width = grad.shape
    f32, bf16 = jnp.float32, jnp.bfloat16
    dp, fs = lax.axis_index("dp"), lax.axis_index("fsdp")
    chip, core = dp // 2, dp % 2
    other = 1 - core
    x, y = chip % 2, chip // 2
    near = (2 * y + 1 - x, 2 * (1 - y) + x)
    far = 2 * (1 - y) + 1 - x
    me = dp * depth + fs
    partner = (2 * chip + other, fs)
    across = tuple((2 * q + core, fs) for q in near + (far,))
    chunks, pieces_ = spans(width, CHUNKS), spans(width, PIECES)
    unit = width // UNITS
    kits = [width - (KITS - p) * unit for p in range(KITS)]
    steps = sorted(
        ((z, b, a, c) for z in range(depth) for b in range(2) for a in range(2) for c in range(2)),
        key=lambda s: -(min(s[0], depth - s[0]) + s[1] + s[2] + s[3] / 4),
    )[:-1]

    def each_other_device(act):
        for dz, b, a, c in steps:
            to_y = 1 - y if b else y
            to_x = 1 - x if a else x
            to_core = other if c else core
            act(((2 * to_y + to_x) * 2 + to_core, (fs + dz) % depth))

    def remote(src, dst, send, recv, to):
        return pltpu.make_async_remote_copy(
            src_ref=src, dst_ref=dst, send_sem=send, recv_sem=recv, device_id=to, device_id_type=MESH
        )

    def settle(ref, sem):
        pltpu.make_async_copy(ref, ref, sem).wait()

    step = lgr.shape[0] // PARTS
    lgr_loads = [
        pltpu.make_async_copy(lgr.at[pl.ds(i * step, step)], lgr_v.at[pl.ds(i * step, step)], lgr_sem.at[i])
        for i in range(PARTS)
    ]
    for load in lgr_loads:
        load.start()
    loads = [
        pltpu.make_async_copy(hid.at[:, pl.ds(start, w)], hid_v[j], hid_sem.at[j])
        for j, (start, w, _) in enumerate(chunks)
    ]
    loads[0].start(priority=1)
    barrier = pltpu.get_barrier_semaphore()
    each_other_device(
        lambda to: pl.semaphore_signal(barrier, inc=1, device_id=to, device_id_type=MESH)
    )
    states = [
        pltpu.make_async_copy(src, dst, state_sem.at[i])
        for i, (src, dst) in enumerate(((mas, mas_v), (one, one_v), (two, two_v)))
    ]

    def pair_copy(j):
        return remote(stage[j].at[other], paired[j], pair_send, pair_recv.at[j], partner)

    def first_copy(j, way):
        return remote(p1_out[j].at[way], p1_in[j].at[way], p1_send.at[j], p1_recv.at[j, way], across[way])

    def second_copy(j, way):
        return remote(p2_out[j].at[way], p2_in[j].at[way], p2_send.at[j], p2_recv.at[j, way], across[way])

    def both(j, q, start, w):
        cols = pl.ds(start, w)
        return stage[j][core, q, :, cols].astype(f32) + paired[j][q, :, cols].astype(f32)

    def chip_sum(j):
        start, w, relayed = chunks[j]
        wh = w // 2
        pair_copy(j).wait_recv()
        if relayed:
            for way in range(2):
                p1_out[j][way, 1] = both(j, far, way * wh, wh).astype(bf16)
                p1_out[j][way, 0] = both(j, near[way], way * wh, wh).astype(bf16)
                first_copy(j, way).start()
        else:
            for way, q in ((2, far), (0, near[0]), (1, near[1])):
                p1_out[j][way] = both(j, q, 0, w).astype(bf16)
                first_copy(j, way).start()
        grad[:, pl.ds(start, w)] = both(j, chip, 0, w)

    loads[1].start(priority=1)
    for i in range(PARTS):
        lgr_loads[i].wait()
        lgt_v[:, i * step : (i + 1) * step] = lgr_v[i * step : (i + 1) * step, :].T
    for load in loads[2:AHEAD]:
        load.start(priority=1)
    for j in range(len(chunks)):
        loads[j].wait()
        if j + AHEAD < len(chunks):
            loads[j + AHEAD].start(priority=1)
        elif j + AHEAD == len(chunks):
            for load in states:
                load.start()
        part = jnp.dot(lgt_v[...], hid_v[j][...], preferred_element_type=f32).astype(bf16)
        for q in range(n // 2):
            for c in range(2):
                d = 2 * q + c
                stage[j][c, q] = part[d * rows : (d + 1) * rows, :]
        if j == 0:
            pl.semaphore_wait(barrier, total - 1)
        pair_copy(j).start()
        if j > 0:
            chip_sum(j - 1)
    chip_sum(len(chunks) - 1)

    def state_copy(p, way):
        return remote(
            kit[p].at[3, pl.ds(0, 3)], kit[p].at[way, pl.ds(0, 3)], kit_send.at[p], kit_recv.at[p, 0, way], across[way]
        )

    def grad_copy(p, way):
        return remote(kit[p].at[3, 3], kit[p].at[way, 3], kit_send.at[p], kit_recv.at[p, 1, way], across[way])

    correct_one, correct_two = 1.0 - 0.9**10, 1.0 - 0.95**10
    for load in states:
        load.wait()
    for p, start in enumerate(kits):
        span = pl.ds(start, unit)
        held = mas_v[:, span]
        kit[p][3, 0] = (held - 0.05 * 0.1 * held).astype(bf16)
        kit[p][3, 1] = (0.05 * 0.9 / correct_one * one_v[:, span]).astype(bf16)
        kit[p][3, 2] = (0.95 / correct_two * two_v[:, span]).astype(bf16)
        if p < EARLY:
            for way in (2, 0, 1):
                state_copy(p, way).start()

    relayed_chunks = [j for j in range(len(chunks)) if chunks[j][2]]
    for j in relayed_chunks:
        wh = chunks[j][1] // 2
        for way in range(2):
            first_copy(j, way).wait_recv()
            away = 1 - way
            joined = both(j, near[away], way * wh, wh) + p1_in[j][way, 1].astype(f32)
            p2_out[j][away] = joined.astype(bf16)
            second_copy(j, away).start()

    squares = jnp.zeros((8, 128), f32)

    def add(start, w, terms, squares):
        span = pl.ds(start, w)
        value = grad[:, span]
        for term in terms:
            value = value + term.astype(f32)
        grad[:, span] = value
        value = value * value
        for r in range(rows // 8):
            for s in range(w // 128):
                squares = squares + value[r * 8 : (r + 1) * 8, s * 128 : (s + 1) * 128]
        return squares

    for j in relayed_chunks:
        start, w, _ = chunks[j]
        wh = w // 2
        for way in range(2):
            second_copy(j, 1 - way).wait_recv()
            squares = add(start + way * wh, wh, (p1_in[j][way, 0], p2_in[j][1 - way]), squares)
    for j, (start, w, relayed) in enumerate(chunks):
        if not relayed:
            for way in range(3):
                first_copy(j, way).wait_recv()
            squares = add(start, w, [p1_in[j][way] for way in range(3)], squares)

    sq_all[me] = jnp.sum(squares, axis=0, keepdims=True)
    each_other_device(
        lambda to: remote(sq_all.at[me], sq_all.at[me], sq_send, sq_recv, to).start()
    )
    for p, start in enumerate(kits):
        kit[p][3, 3] = grad[:, pl.ds(start, unit)].astype(bf16)
        if p < EARLY:
            for way in (2, 0, 1):
                grad_copy(p, way).start()
    for p in range(EARLY, KITS):
        for way in (2, 0, 1):
            state_copy(p, way).start()
        for way in (2, 0, 1):
            grad_copy(p, way).start()
    everyone = sq_all.at[pl.ds(0, total - 1)]
    settle(everyone, sq_recv)
    sumsq = jnp.sum(jnp.sum(sq_all[...], axis=0), axis=1, keepdims=True)
    rms = jnp.sqrt(sumsq / (rows * n * width * depth))
    factor = jnp.where(rms > 1.0, 1.0 / rms, 1.0)

    def block(q, start, w):
        return rows_out.at[pl.ds(pl.multiple_of((2 * q + core) * rows, rows), rows), pl.ds(start, w)]

    def own_copy(k, way, q):
        start, w, relayed = pieces_[k]
        sem = ag_send.at[0 if relayed else 1]
        return remote(block(q, start, w), block(q, start, w), sem, ag_recv.at[k, way], across[way])

    def far_copy(k, way, q):
        start, w, _ = pieces_[k]
        part = block(q, start + way * (w // 2), w // 2)
        return remote(part, part, far_send, far_recv.at[k, way], across[1 - way])

    def relay(q, start, w):
        return remote(block(q, start, w), block(q, start, w), relay_send, relay_recv, partner)

    def update(start, w):
        span = pl.ds(start, w)
        clipped = factor * grad[:, span]
        new_one = 0.9 * one_v[:, span] + 0.1 * clipped
        new_two = 0.95 * two_v[:, span] + 0.05 * clipped * clipped
        first = new_one / correct_one
        second = new_two / correct_two
        held = mas_v[:, span]
        new_master = held - 0.05 * (first / (jnp.sqrt(second) + 1e-08) + 0.1 * held)
        one_out[:, span] = new_one
        two_out[:, span] = new_two
        mas_out[:, span] = new_master
        return new_master

    def rows_of(d):
        return pl.ds(pl.multiple_of(d * rows, rows), rows)

    for k, (start, w, relayed) in enumerate(pieces_):
        rows_out[rows_of(dp), pl.ds(start, w)] = update(start, w).astype(bf16)
        for way in (0, 1) if relayed else (2, 0, 1):
            own_copy(k, way, chip).start()
        relay(chip, start, w).start()
    for p, start in enumerate(kits):
        update(start, unit)
        for way in range(3):
            state_copy(p, way).wait_recv()
            grad_copy(p, way).wait_recv()
        for slot, q in enumerate(near + (far, chip)):
            base, step_one, step_two, part = (kit[p][slot, i].astype(f32) for i in range(4))
            clipped = factor * part
            step_one = step_one + 0.05 * 0.1 / correct_one * clipped
            step_two = step_two + 0.05 / correct_two * clipped * clipped
            new_rows = base - step_one / (jnp.sqrt(step_two) + 1e-08)
            rows_out[rows_of(2 * q + core), pl.ds(start, unit)] = new_rows.astype(bf16)
            relay(q, start, unit).start()

    for k, (start, w, relayed) in enumerate(pieces_):
        if relayed:
            for way in range(2):
                own_copy(k, way, near[way]).wait_recv()
                far_copy(k, way, near[way]).start()
                relay(near[way], start, w).start()
    for k, (start, w, relayed) in enumerate(pieces_):
        if not relayed:
            for way, q in ((0, near[0]), (1, near[1]), (2, far)):
                own_copy(k, way, q).wait_recv()
                relay(q, start, w).start()
    for k, (start, w, relayed) in enumerate(pieces_):
        if relayed:
            for way in range(2):
                far_copy(k, way, far).wait_recv()
                relay(far, start + way * (w // 2), w // 2).start()

    for j, (_, w, relayed) in enumerate(chunks):
        settle(paired[j], pair_send)
        settle(p1_in[j], p1_send.at[j])
        if relayed:
            settle(p2_in[j], p2_send.at[j])
    settle(everyone, sq_send)
    sent = sum(w for _, w, relayed in pieces_ if relayed)
    settle(rows_out.at[pl.ds(0, 2 * rows), pl.ds(0, sent)], ag_send.at[0])
    settle(rows_out.at[pl.ds(0, rows), pl.ds(0, sent)], far_send)
    straight = width - KITS * unit - sent
    if straight > 0:
        settle(rows_out.at[pl.ds(0, 3 * rows), pl.ds(0, straight)], ag_send.at[1])
    for p in range(KITS):
        settle(kit[p].at[pl.ds(0, 3)], kit_send.at[p])
    settle(rows_out.at[pl.ds(0, 4 * rows)], relay_send)
    settle(rows_out.at[pl.ds(0, 4 * rows)], relay_recv)


def write_out(*refs):
    sems = refs[8]
    copies = [pltpu.make_async_copy(refs[i], refs[4 + i], sems.at[i]) for i in range(4)]
    for copy in copies:
        copy.start()
    for copy in copies:
        copy.wait()


def shards(n, depth, hidden, logit_grad, master, moment_one, moment_two):
    tokens, width = hidden.shape
    slab = logit_grad.shape[1]
    rows = master.shape[0]
    chips = n // 2
    f32, bf16 = jnp.float32, jnp.bfloat16
    state = ((rows, width), f32)
    shapes = (((slab, width), bf16), state, state, state)
    kept = slab * width * 2 + 3 * rows * width * 4
    dma = pltpu.SemaphoreType.DMA
    anywhere = pl.BlockSpec(memory_space=pl.ANY)
    in_vmem = pl.BlockSpec(memory_space=pltpu.VMEM)
    if n == 8 and width % (UNITS * 256) == 0 and tokens % (PARTS * 128) == 0:
        body = functools.partial(square_kernel, n, depth)
        scratch = square_scratch(n, depth, tokens, slab, rows, width)
    else:
        chunks = pieces(width, LOAD_CHUNKS)
        gathers = pieces(width, GATHER_CHUNKS)
        wc = width // chunks
        body = functools.partial(direct_kernel, n, depth, chunks, gathers)
        scratch = [
            pltpu.VMEM((tokens, slab), bf16),
            pltpu.VMEM((slab, tokens), bf16),
            pltpu.VMEM((chunks, tokens, wc), bf16),
            pltpu.VMEM((rows, width), f32),
            pltpu.VMEM((rows, width), f32),
            pltpu.VMEM((rows, width), f32),
            pltpu.VMEM((chunks, 2, chips, rows, wc), bf16),
            pltpu.VMEM((chunks, chips, rows, wc), bf16),
            pltpu.VMEM((chunks, chips, rows, wc), bf16),
            pltpu.VMEM((chunks, chips, rows, wc), bf16),
            pltpu.VMEM((rows, width), f32),
            pltpu.VMEM((n * depth, 1, 128), f32),
            dma((chunks,)),
            dma,
            dma((3,)),
            dma((chunks,)),
            dma((chunks,)),
            dma((chunks, chips)),
            dma((chunks, chips)),
            dma,
            dma,
            dma((gathers, chips)),
            dma((gathers, chips)),
            dma((gathers, chips)),
            dma((gathers, chips)),
        ]
    held = pl.pallas_call(
        body,
        out_shape=tuple(pltpu.VMEM(*shape) for shape in shapes),
        in_specs=[anywhere] * 5,
        out_specs=(in_vmem,) * 4,
        scratch_shapes=scratch,
        compiler_params=pltpu.CompilerParams(
            collective_id=0, has_side_effects=True, vmem_limit_bytes=VMEM_BYTES - kept - 96 * 1024
        ),
    )(hidden, logit_grad, master, moment_one, moment_two)
    return pl.pallas_call(
        write_out,
        out_shape=tuple(pltpu.HBM(*shape) for shape in shapes),
        in_specs=[anywhere] * 4,
        out_specs=(anywhere,) * 4,
        scratch_shapes=[dma((4,))],
        compiler_params=pltpu.CompilerParams(vmem_limit_bytes=1024 * 1024),
    )(*held)


def solution(mesh):
    placed = (P("dp", "fsdp"), P("dp", None), P("dp", "fsdp"), P("dp", "fsdp"), P("dp", "fsdp"))
    return jax.shard_map(
        functools.partial(shards, mesh.shape["dp"], mesh.shape["fsdp"]),
        mesh=mesh,
        in_specs=placed,
        out_specs=(P(None, "fsdp"), P("dp", "fsdp"), P("dp", "fsdp"), P("dp", "fsdp")),
        check_vma=False,
    )
```

```python
import functools

import jax
import jax.numpy as jnp
from jax import lax
from jax.experimental import pallas as pl
from jax.experimental.pallas import tpu as pltpu
from jax.sharding import PartitionSpec as P

MESH = pl.DeviceIdType.MESH
LOAD_CHUNKS = 4
GATHER_CHUNKS = 2
VMEM_BYTES = 67_043_328
UNITS = 8
PARTS = 4
CHUNKS = ((2, True), (2, True), (2, False), (2, False))
PIECES = ((2, True), (3, False), (2, False))
KITS = 1
EARLY = 0
AHEAD = 2


def pieces(width, wanted):
    count = wanted
    while count > 1 and width % (count * 128):
        count -= 1
    return count


def direct_kernel(
    n, depth, chunks, gathers,
    hid, lgr, mas, one, two,
    rows_out, mas_out, one_out, two_out,
    lgr_v, lgt_v, hid_v, mas_v, one_v, two_v,
    stage, paired, sums, arrived, grad, sq_all,
    hid_sem, lgr_sem, state_sem, pair_send, pair_recv, chip_send, chip_recv,
    sq_send, sq_recv, ag_send, ag_recv, relay_send, relay_recv,
):
    chips = n // 2
    total = n * depth
    rows, width = grad.shape
    dp, fs = lax.axis_index("dp"), lax.axis_index("fsdp")
    chip, core = dp // 2, dp % 2
    other = 1 - core
    me = dp * depth + fs
    wc, wa = width // chunks, width // gathers

    lgr_copy = pltpu.make_async_copy(lgr, lgr_v, lgr_sem)
    lgr_copy.start()
    loads = []
    for j in range(chunks):
        load = pltpu.make_async_copy(hid.at[:, pl.ds(j * wc, wc)], hid_v.at[j], hid_sem.at[j])
        load.start()
        loads.append(load)
    states = []
    for i, (src, dst) in enumerate(((mas, mas_v), (one, one_v), (two, two_v))):
        load = pltpu.make_async_copy(src, dst, state_sem.at[i])
        load.start()
        states.append(load)

    def each_other_device(act):
        def visit(i):
            index = (me + i) % total
            act((index // depth, index % depth))

        if total <= 64:
            for i in range(1, total):
                visit(i)
        else:
            lax.fori_loop(1, total, lambda i, carry: (visit(i), carry)[1], 0)

    barrier = pltpu.get_barrier_semaphore()
    each_other_device(
        lambda to: pl.semaphore_signal(barrier, inc=1, device_id=to, device_id_type=MESH)
    )

    lgr_copy.wait()
    lgt_v[...] = lgr_v[...].T

    def remote(src, dst, send, recv, to):
        return pltpu.make_async_remote_copy(
            src_ref=src, dst_ref=dst, send_sem=send, recv_sem=recv, device_id=to, device_id_type=MESH
        )

    partner = (2 * chip + other, fs)
    others = [(chip + o) % chips for o in range(1, chips)]

    def pair_copy(j):
        return remote(stage.at[j, other], paired.at[j], pair_send.at[j], pair_recv.at[j], partner)

    def chip_copy(j, q, slot):
        return remote(
            sums.at[j, q], arrived.at[j, slot], chip_send.at[j, q], chip_recv.at[j, slot],
            (2 * q + core, fs),
        )

    def chip_sum(j):
        pair_copy(j).wait_recv()
        for q in others:
            both = stage[j, core, q].astype(jnp.float32) + paired[j, q].astype(jnp.float32)
            sums[j, q] = both.astype(jnp.bfloat16)
            chip_copy(j, q, chip).start()
        grad[:, pl.ds(j * wc, wc)] = stage[j, core, chip].astype(jnp.float32) + paired[
            j, chip
        ].astype(jnp.float32)

    for j in range(chunks):
        loads[j].wait()
        part = jnp.dot(lgt_v[...], hid_v[j], preferred_element_type=jnp.float32)
        part = part.astype(jnp.bfloat16)
        for q in range(chips):
            for c in range(2):
                d = 2 * q + c
                stage[j, c, q] = part[d * rows : (d + 1) * rows, :]
        if j == 0:
            pl.semaphore_wait(barrier, total - 1)
        pair_copy(j).start()
        if j > 0:
            chip_sum(j - 1)
    chip_sum(chunks - 1)

    squares = jnp.zeros((1, 128), jnp.float32)
    for j in range(chunks):
        span = pl.ds(j * wc, wc)
        value = grad[:, span]
        for q in others:
            chip_copy(j, q, q).wait_recv()
            value = value + arrived[j, q].astype(jnp.float32)
        grad[:, span] = value
        column = jnp.sum(value * value, axis=0, keepdims=True)
        for s in range(wc // 128):
            squares = squares + column[:, s * 128 : (s + 1) * 128]

    sq_all[me] = squares
    each_other_device(
        lambda to: remote(sq_all.at[me], sq_all.at[me], sq_send, sq_recv, to).start()
    )
    for load in states:
        load.wait()
    everyone = sq_all.at[pl.ds(0, total - 1)]
    pltpu.make_async_copy(everyone, everyone, sq_recv).wait()
    sumsq = jnp.sum(jnp.sum(sq_all[...], axis=0), axis=1, keepdims=True)
    rms = jnp.sqrt(sumsq / (rows * n * width * depth))
    factor = jnp.where(rms > 1.0, 1.0 / rms, 1.0)

    def cols(k):
        return pl.ds(k * wa, wa)

    def rows_of(d):
        return pl.ds(pl.multiple_of(d * rows, rows), rows)

    def gather_copy(k, d, to, send, recv):
        block = rows_out.at[rows_of(d), cols(k)]
        return remote(block, block, send, recv, to)

    def direct(k, source, q):
        return gather_copy(k, 2 * source + core, (2 * q + core, fs), ag_send.at[k, q], ag_recv.at[k, source])

    def relay(k, q, side):
        return gather_copy(k, 2 * q + side, partner, relay_send.at[k, q], relay_recv.at[k, q])

    for k in range(gathers):
        span = cols(k)
        clipped = factor * grad[:, span]
        new_one = 0.9 * one_v[:, span] + 0.1 * clipped
        new_two = 0.95 * two_v[:, span] + 0.05 * clipped * clipped
        first = new_one / (1.0 - 0.9**10)
        second = new_two / (1.0 - 0.95**10)
        held = mas_v[:, span]
        new_master = held - 0.05 * (first / (jnp.sqrt(second) + 1e-08) + 0.1 * held)
        rows_out[rows_of(dp), span] = new_master.astype(jnp.bfloat16)
        for q in others:
            direct(k, chip, q).start()
        relay(k, chip, core).start()
        one_out[:, span] = new_one
        two_out[:, span] = new_two
        mas_out[:, span] = new_master
    for k in range(gathers):
        for q in others:
            direct(k, q, q).wait_recv()
            relay(k, q, core).start()
    for k in range(gathers):
        for q in [chip] + others:
            relay(k, q, other).wait_recv()

    for j in range(chunks):
        pair_copy(j).wait_send()
        for q in others:
            chip_copy(j, q, chip).wait_send()
    pltpu.make_async_copy(everyone, everyone, sq_send).wait()
    for k in range(gathers):
        for q in others:
            direct(k, chip, q).wait_send()
            relay(k, q, core).wait_send()
        relay(k, chip, core).wait_send()


def spans(width, plan):
    unit, start, result = width // UNITS, 0, []
    for count, relayed in plan:
        result.append((start, count * unit, relayed))
        start += count * unit
    return result


def square_scratch(n, depth, tokens, slab, rows, width):
    f32, bf16 = jnp.float32, jnp.bfloat16
    dma = pltpu.SemaphoreType.DMA
    chunks = [(w, relayed) for _, w, relayed in spans(width, CHUNKS)]
    state = pltpu.VMEM((rows, width), f32)
    stage = tuple(pltpu.VMEM((2, n // 2, rows, w), bf16) for w, _ in chunks)
    paired = tuple(pltpu.VMEM((n // 2, rows, w), bf16) for w, _ in chunks)
    first = tuple(
        pltpu.VMEM((2, 2, rows, w // 2) if relayed else (3, rows, w), bf16) for w, relayed in chunks
    )
    second = tuple(pltpu.VMEM((2, rows, w // 2), bf16) for w, _ in chunks)
    many = len(chunks)
    return [
        pltpu.VMEM((tokens, slab), bf16),
        pltpu.VMEM((slab, tokens), bf16),
        tuple(pltpu.VMEM((tokens, w), bf16) for w, _ in chunks),
        state, state, state, state,
        stage, paired, first, first, second, second,
        tuple(pltpu.VMEM((4, 4, rows, width // UNITS), bf16) for _ in range(KITS)),
        pltpu.VMEM((n * depth, 1, 128), f32),
        dma((PARTS,)), dma((many,)), dma((3,)),
        dma, dma((many,)),
        dma((many,)), dma((many, 3)),
        dma((many,)), dma((many, 2)),
        dma, dma,
        dma((2,)), dma((len(PIECES), 3)),
        dma, dma((len(PIECES), 2)),
        dma, dma,
        dma((KITS,)), dma((KITS, 2, 3)),
    ]


def square_kernel(
    n, depth,
    hid, lgr, mas, one, two,
    rows_out, mas_out, one_out, two_out,
    lgr_v, lgt_v, hid_v, mas_v, one_v, two_v, grad,
    stage, paired, p1_out, p1_in, p2_out, p2_in, kit, sq_all,
    lgr_sem, hid_sem, state_sem, pair_send, pair_recv, p1_send, p1_recv, p2_send, p2_recv,
    sq_send, sq_recv, ag_send, ag_recv, far_send, far_recv, relay_send, relay_recv,
    kit_send, kit_recv,
):
    total = n * depth
    rows, width = grad.shape
    f32, bf16 = jnp.float32, jnp.bfloat16
    dp, fs = lax.axis_index("dp"), lax.axis_index("fsdp")
    chip, core = dp // 2, dp % 2
    other = 1 - core
    x, y = chip % 2, chip // 2
    near = (2 * y + 1 - x, 2 * (1 - y) + x)
    far = 2 * (1 - y) + 1 - x
    me = dp * depth + fs
    partner = (2 * chip + other, fs)
    across = tuple((2 * q + core, fs) for q in near + (far,))
    chunks, pieces_ = spans(width, CHUNKS), spans(width, PIECES)
    unit = width // UNITS
    kits = [width - (KITS - p) * unit for p in range(KITS)]
    steps = sorted(
        ((z, b, a, c) for z in range(depth) for b in range(2) for a in range(2) for c in range(2)),
        key=lambda s: -(min(s[0], depth - s[0]) + s[1] + s[2] + s[3] / 4),
    )[:-1]

    def each_other_device(act):
        for dz, b, a, c in steps:
            to_y = 1 - y if b else y
            to_x = 1 - x if a else x
            to_core = other if c else core
            act(((2 * to_y + to_x) * 2 + to_core, (fs + dz) % depth))

    def remote(src, dst, send, recv, to):
        return pltpu.make_async_remote_copy(
            src_ref=src, dst_ref=dst, send_sem=send, recv_sem=recv, device_id=to, device_id_type=MESH
        )

    def settle(ref, sem):
        pltpu.make_async_copy(ref, ref, sem).wait()

    step = lgr.shape[0] // PARTS
    lgr_loads = [
        pltpu.make_async_copy(lgr.at[pl.ds(i * step, step)], lgr_v.at[pl.ds(i * step, step)], lgr_sem.at[i])
        for i in range(PARTS)
    ]
    for load in lgr_loads:
        load.start()
    loads = [
        pltpu.make_async_copy(hid.at[:, pl.ds(start, w)], hid_v[j], hid_sem.at[j])
        for j, (start, w, _) in enumerate(chunks)
    ]
    loads[0].start(priority=1)
    barrier = pltpu.get_barrier_semaphore()
    each_other_device(
        lambda to: pl.semaphore_signal(barrier, inc=1, device_id=to, device_id_type=MESH)
    )
    states = [
        pltpu.make_async_copy(src, dst, state_sem.at[i])
        for i, (src, dst) in enumerate(((mas, mas_v), (one, one_v), (two, two_v)))
    ]

    def pair_copy(j):
        return remote(stage[j].at[other], paired[j], pair_send, pair_recv.at[j], partner)

    def first_copy(j, way):
        return remote(p1_out[j].at[way], p1_in[j].at[way], p1_send.at[j], p1_recv.at[j, way], across[way])

    def second_copy(j, way):
        return remote(p2_out[j].at[way], p2_in[j].at[way], p2_send.at[j], p2_recv.at[j, way], across[way])

    def both(j, q, start, w):
        cols = pl.ds(start, w)
        return stage[j][core, q, :, cols].astype(f32) + paired[j][q, :, cols].astype(f32)

    def chip_sum(j):
        start, w, relayed = chunks[j]
        wh = w // 2
        pair_copy(j).wait_recv()
        if relayed:
            for way in range(2):
                p1_out[j][way, 1] = both(j, far, way * wh, wh).astype(bf16)
                p1_out[j][way, 0] = both(j, near[way], way * wh, wh).astype(bf16)
                first_copy(j, way).start()
        else:
            for way, q in ((2, far), (0, near[0]), (1, near[1])):
                p1_out[j][way] = both(j, q, 0, w).astype(bf16)
                first_copy(j, way).start()
        grad[:, pl.ds(start, w)] = both(j, chip, 0, w)

    loads[1].start(priority=1)
    for i in range(PARTS):
        lgr_loads[i].wait()
        lgt_v[:, i * step : (i + 1) * step] = lgr_v[i * step : (i + 1) * step, :].T
    for load in loads[2:AHEAD]:
        load.start(priority=1)
    for j in range(len(chunks)):
        loads[j].wait()
        if j + AHEAD < len(chunks):
            loads[j + AHEAD].start(priority=1)
        elif j + AHEAD == len(chunks):
            for load in states:
                load.start()
        part = jnp.dot(lgt_v[...], hid_v[j][...], preferred_element_type=f32).astype(bf16)
        for q in range(n // 2):
            for c in range(2):
                d = 2 * q + c
                stage[j][c, q] = part[d * rows : (d + 1) * rows, :]
        if j == 0:
            pl.semaphore_wait(barrier, total - 1)
        pair_copy(j).start()
        if j > 0:
            chip_sum(j - 1)
    chip_sum(len(chunks) - 1)

    def state_copy(p, way):
        return remote(
            kit[p].at[3, pl.ds(0, 3)], kit[p].at[way, pl.ds(0, 3)], kit_send.at[p], kit_recv.at[p, 0, way], across[way]
        )

    def grad_copy(p, way):
        return remote(kit[p].at[3, 3], kit[p].at[way, 3], kit_send.at[p], kit_recv.at[p, 1, way], across[way])

    correct_one, correct_two = 1.0 - 0.9**10, 1.0 - 0.95**10
    for load in states:
        load.wait()
    for p, start in enumerate(kits):
        span = pl.ds(start, unit)
        held = mas_v[:, span]
        kit[p][3, 0] = (held - 0.05 * 0.1 * held).astype(bf16)
        kit[p][3, 1] = (0.05 * 0.9 / correct_one * one_v[:, span]).astype(bf16)
        kit[p][3, 2] = (0.95 / correct_two * two_v[:, span]).astype(bf16)
        if p < EARLY:
            for way in (2, 0, 1):
                state_copy(p, way).start()

    relayed_chunks = [j for j in range(len(chunks)) if chunks[j][2]]
    for j in relayed_chunks:
        wh = chunks[j][1] // 2
        for way in range(2):
            first_copy(j, way).wait_recv()
            away = 1 - way
            joined = both(j, near[away], way * wh, wh) + p1_in[j][way, 1].astype(f32)
            p2_out[j][away] = joined.astype(bf16)
            second_copy(j, away).start()

    squares = jnp.zeros((8, 128), f32)

    def add(start, w, terms, squares):
        span = pl.ds(start, w)
        value = grad[:, span]
        for term in terms:
            value = value + term.astype(f32)
        grad[:, span] = value
        value = value * value
        for r in range(rows // 8):
            for s in range(w // 128):
                squares = squares + value[r * 8 : (r + 1) * 8, s * 128 : (s + 1) * 128]
        return squares

    for j in relayed_chunks:
        start, w, _ = chunks[j]
        wh = w // 2
        for way in range(2):
            second_copy(j, 1 - way).wait_recv()
            squares = add(start + way * wh, wh, (p1_in[j][way, 0], p2_in[j][1 - way]), squares)
    for j, (start, w, relayed) in enumerate(chunks):
        if not relayed:
            for way in range(3):
                first_copy(j, way).wait_recv()
            squares = add(start, w, [p1_in[j][way] for way in range(3)], squares)

    sq_all[me] = jnp.sum(squares, axis=0, keepdims=True)
    def tell(to_y, to_x, to_core, to_z):
        to = ((2 * to_y + to_x) * 2 + to_core, to_z)
        remote(sq_all.at[me], sq_all.at[me], sq_send, sq_recv, to).start()

    for to_z in range(depth):
        for to_y, to_x, to_core in (
            (1 - y, 1 - x, other), (1 - y, 1 - x, core), (1 - y, x, other), (y, 1 - x, other),
            (1 - y, x, core), (y, 1 - x, core), (y, x, other),
        ):
            tell(to_y, to_x, to_core, to_z)
    for dz in range(1, depth):
        tell(y, x, core, (fs + dz) % depth)
    for p, start in enumerate(kits):
        kit[p][3, 3] = grad[:, pl.ds(start, unit)].astype(bf16)
        if p < EARLY:
            for way in (2, 0, 1):
                grad_copy(p, way).start()
    for p in range(EARLY, KITS):
        for way in (2, 0, 1):
            state_copy(p, way).start()
        for way in (2, 0, 1):
            grad_copy(p, way).start()
    everyone = sq_all.at[pl.ds(0, total - 1)]
    settle(everyone, sq_recv)
    sumsq = jnp.sum(jnp.sum(sq_all[...], axis=0), axis=1, keepdims=True)
    rms = jnp.sqrt(sumsq / (rows * n * width * depth))
    factor = jnp.where(rms > 1.0, 1.0 / rms, 1.0)

    def block(q, start, w):
        return rows_out.at[pl.ds(pl.multiple_of((2 * q + core) * rows, rows), rows), pl.ds(start, w)]

    def own_copy(k, way, q):
        start, w, relayed = pieces_[k]
        sem = ag_send.at[0 if relayed else 1]
        return remote(block(q, start, w), block(q, start, w), sem, ag_recv.at[k, way], across[way])

    def far_copy(k, way, q):
        start, w, _ = pieces_[k]
        part = block(q, start + way * (w // 2), w // 2)
        return remote(part, part, far_send, far_recv.at[k, way], across[1 - way])

    def relay(q, start, w):
        return remote(block(q, start, w), block(q, start, w), relay_send, relay_recv, partner)

    def update(start, w):
        span = pl.ds(start, w)
        clipped = factor * grad[:, span]
        new_one = 0.9 * one_v[:, span] + 0.1 * clipped
        new_two = 0.95 * two_v[:, span] + 0.05 * clipped * clipped
        first = new_one / correct_one
        second = new_two / correct_two
        held = mas_v[:, span]
        new_master = held - 0.05 * (first / (jnp.sqrt(second) + 1e-08) + 0.1 * held)
        one_out[:, span] = new_one
        two_out[:, span] = new_two
        mas_out[:, span] = new_master
        return new_master

    def rows_of(d):
        return pl.ds(pl.multiple_of(d * rows, rows), rows)

    for k, (start, w, relayed) in enumerate(pieces_):
        rows_out[rows_of(dp), pl.ds(start, w)] = update(start, w).astype(bf16)
        for way in (0, 1) if relayed else (2, 0, 1):
            own_copy(k, way, chip).start()
        relay(chip, start, w).start()
    for p, start in enumerate(kits):
        update(start, unit)
        for way in range(3):
            state_copy(p, way).wait_recv()
            grad_copy(p, way).wait_recv()
        for slot, q in enumerate(near + (far, chip)):
            base, step_one, step_two, part = (kit[p][slot, i].astype(f32) for i in range(4))
            clipped = factor * part
            step_one = step_one + 0.05 * 0.1 / correct_one * clipped
            step_two = step_two + 0.05 / correct_two * clipped * clipped
            new_rows = base - step_one / (jnp.sqrt(step_two) + 1e-08)
            rows_out[rows_of(2 * q + core), pl.ds(start, unit)] = new_rows.astype(bf16)
            relay(q, start, unit).start()

    for k, (start, w, relayed) in enumerate(pieces_):
        if relayed:
            for way in range(2):
                own_copy(k, way, near[way]).wait_recv()
                far_copy(k, way, near[way]).start()
                relay(near[way], start, w).start()
    for k, (start, w, relayed) in enumerate(pieces_):
        if not relayed:
            for way, q in ((0, near[0]), (1, near[1]), (2, far)):
                own_copy(k, way, q).wait_recv()
                relay(q, start, w).start()
    for k, (start, w, relayed) in enumerate(pieces_):
        if relayed:
            for way in range(2):
                far_copy(k, way, far).wait_recv()
                relay(far, start + way * (w // 2), w // 2).start()

    for j, (_, w, relayed) in enumerate(chunks):
        settle(paired[j], pair_send)
        settle(p1_in[j], p1_send.at[j])
        if relayed:
            settle(p2_in[j], p2_send.at[j])
    settle(everyone, sq_send)
    sent = sum(w for _, w, relayed in pieces_ if relayed)
    settle(rows_out.at[pl.ds(0, 2 * rows), pl.ds(0, sent)], ag_send.at[0])
    settle(rows_out.at[pl.ds(0, rows), pl.ds(0, sent)], far_send)
    straight = width - KITS * unit - sent
    if straight > 0:
        settle(rows_out.at[pl.ds(0, 3 * rows), pl.ds(0, straight)], ag_send.at[1])
    for p in range(KITS):
        settle(kit[p].at[pl.ds(0, 3)], kit_send.at[p])
    settle(rows_out.at[pl.ds(0, 4 * rows)], relay_send)
    settle(rows_out.at[pl.ds(0, 4 * rows)], relay_recv)


def write_out(*refs):
    sems = refs[8]
    copies = [pltpu.make_async_copy(refs[i], refs[4 + i], sems.at[i]) for i in range(4)]
    for copy in copies:
        copy.start()
    for copy in copies:
        copy.wait()


def shards(n, depth, hidden, logit_grad, master, moment_one, moment_two):
    tokens, width = hidden.shape
    slab = logit_grad.shape[1]
    rows = master.shape[0]
    chips = n // 2
    f32, bf16 = jnp.float32, jnp.bfloat16
    state = ((rows, width), f32)
    shapes = (((slab, width), bf16), state, state, state)
    kept = slab * width * 2 + 3 * rows * width * 4
    dma = pltpu.SemaphoreType.DMA
    anywhere = pl.BlockSpec(memory_space=pl.ANY)
    in_vmem = pl.BlockSpec(memory_space=pltpu.VMEM)
    if n == 8 and width % (UNITS * 256) == 0 and tokens % (PARTS * 128) == 0:
        body = functools.partial(square_kernel, n, depth)
        scratch = square_scratch(n, depth, tokens, slab, rows, width)
    else:
        chunks = pieces(width, LOAD_CHUNKS)
        gathers = pieces(width, GATHER_CHUNKS)
        wc = width // chunks
        body = functools.partial(direct_kernel, n, depth, chunks, gathers)
        scratch = [
            pltpu.VMEM((tokens, slab), bf16),
            pltpu.VMEM((slab, tokens), bf16),
            pltpu.VMEM((chunks, tokens, wc), bf16),
            pltpu.VMEM((rows, width), f32),
            pltpu.VMEM((rows, width), f32),
            pltpu.VMEM((rows, width), f32),
            pltpu.VMEM((chunks, 2, chips, rows, wc), bf16),
            pltpu.VMEM((chunks, chips, rows, wc), bf16),
            pltpu.VMEM((chunks, chips, rows, wc), bf16),
            pltpu.VMEM((chunks, chips, rows, wc), bf16),
            pltpu.VMEM((rows, width), f32),
            pltpu.VMEM((n * depth, 1, 128), f32),
            dma((chunks,)),
            dma,
            dma((3,)),
            dma((chunks,)),
            dma((chunks,)),
            dma((chunks, chips)),
            dma((chunks, chips)),
            dma,
            dma,
            dma((gathers, chips)),
            dma((gathers, chips)),
            dma((gathers, chips)),
            dma((gathers, chips)),
        ]
    held = pl.pallas_call(
        body,
        out_shape=tuple(pltpu.VMEM(*shape) for shape in shapes),
        in_specs=[anywhere] * 5,
        out_specs=(in_vmem,) * 4,
        scratch_shapes=scratch,
        compiler_params=pltpu.CompilerParams(
            collective_id=0, has_side_effects=True, vmem_limit_bytes=VMEM_BYTES - kept - 96 * 1024
        ),
    )(hidden, logit_grad, master, moment_one, moment_two)
    return pl.pallas_call(
        write_out,
        out_shape=tuple(pltpu.HBM(*shape) for shape in shapes),
        in_specs=[anywhere] * 4,
        out_specs=(anywhere,) * 4,
        scratch_shapes=[dma((4,))],
        compiler_params=pltpu.CompilerParams(vmem_limit_bytes=1024 * 1024),
    )(*held)


def solution(mesh):
    placed = (P("dp", "fsdp"), P("dp", None), P("dp", "fsdp"), P("dp", "fsdp"), P("dp", "fsdp"))
    return jax.shard_map(
        functools.partial(shards, mesh.shape["dp"], mesh.shape["fsdp"]),
        mesh=mesh,
        in_specs=placed,
        out_specs=(P(None, "fsdp"), P("dp", "fsdp"), P("dp", "fsdp"), P("dp", "fsdp")),
        check_vma=False,
    )
```

```python
import functools

import jax
import jax.numpy as jnp
from jax import lax
from jax.experimental import pallas as pl
from jax.experimental.pallas import tpu as pltpu
from jax.sharding import PartitionSpec as P

MESH = pl.DeviceIdType.MESH
LOAD_CHUNKS = 4
GATHER_CHUNKS = 2
VMEM_BYTES = 67_043_328
UNITS = 8
PARTS = 4
CHUNKS = ((2, True), (2, True), (2, False), (2, False))
PIECES = ((2, True), (3, False), (2, False))
KITS = 1
EARLY = 0
AHEAD = 2


def pieces(width, wanted):
    count = wanted
    while count > 1 and width % (count * 128):
        count -= 1
    return count


def direct_kernel(
    n, depth, chunks, gathers,
    hid, lgr, mas, one, two,
    rows_out, mas_out, one_out, two_out,
    lgr_v, lgt_v, hid_v, mas_v, one_v, two_v,
    stage, paired, sums, arrived, grad, sq_all,
    hid_sem, lgr_sem, state_sem, pair_send, pair_recv, chip_send, chip_recv,
    sq_send, sq_recv, ag_send, ag_recv, relay_send, relay_recv,
):
    chips = n // 2
    total = n * depth
    rows, width = grad.shape
    dp, fs = lax.axis_index("dp"), lax.axis_index("fsdp")
    chip, core = dp // 2, dp % 2
    other = 1 - core
    me = dp * depth + fs
    wc, wa = width // chunks, width // gathers

    lgr_copy = pltpu.make_async_copy(lgr, lgr_v, lgr_sem)
    lgr_copy.start()
    loads = []
    for j in range(chunks):
        load = pltpu.make_async_copy(hid.at[:, pl.ds(j * wc, wc)], hid_v.at[j], hid_sem.at[j])
        load.start()
        loads.append(load)
    states = []
    for i, (src, dst) in enumerate(((mas, mas_v), (one, one_v), (two, two_v))):
        load = pltpu.make_async_copy(src, dst, state_sem.at[i])
        load.start()
        states.append(load)

    def each_other_device(act):
        def visit(i):
            index = (me + i) % total
            act((index // depth, index % depth))

        if total <= 64:
            for i in range(1, total):
                visit(i)
        else:
            lax.fori_loop(1, total, lambda i, carry: (visit(i), carry)[1], 0)

    barrier = pltpu.get_barrier_semaphore()
    each_other_device(
        lambda to: pl.semaphore_signal(barrier, inc=1, device_id=to, device_id_type=MESH)
    )

    lgr_copy.wait()
    lgt_v[...] = lgr_v[...].T

    def remote(src, dst, send, recv, to):
        return pltpu.make_async_remote_copy(
            src_ref=src, dst_ref=dst, send_sem=send, recv_sem=recv, device_id=to, device_id_type=MESH
        )

    partner = (2 * chip + other, fs)
    others = [(chip + o) % chips for o in range(1, chips)]

    def pair_copy(j):
        return remote(stage.at[j, other], paired.at[j], pair_send.at[j], pair_recv.at[j], partner)

    def chip_copy(j, q, slot):
        return remote(
            sums.at[j, q], arrived.at[j, slot], chip_send.at[j, q], chip_recv.at[j, slot],
            (2 * q + core, fs),
        )

    def chip_sum(j):
        pair_copy(j).wait_recv()
        for q in others:
            both = stage[j, core, q].astype(jnp.float32) + paired[j, q].astype(jnp.float32)
            sums[j, q] = both.astype(jnp.bfloat16)
            chip_copy(j, q, chip).start()
        grad[:, pl.ds(j * wc, wc)] = stage[j, core, chip].astype(jnp.float32) + paired[
            j, chip
        ].astype(jnp.float32)

    for j in range(chunks):
        loads[j].wait()
        part = jnp.dot(lgt_v[...], hid_v[j], preferred_element_type=jnp.float32)
        part = part.astype(jnp.bfloat16)
        for q in range(chips):
            for c in range(2):
                d = 2 * q + c
                stage[j, c, q] = part[d * rows : (d + 1) * rows, :]
        if j == 0:
            pl.semaphore_wait(barrier, total - 1)
        pair_copy(j).start()
        if j > 0:
            chip_sum(j - 1)
    chip_sum(chunks - 1)

    squares = jnp.zeros((1, 128), jnp.float32)
    for j in range(chunks):
        span = pl.ds(j * wc, wc)
        value = grad[:, span]
        for q in others:
            chip_copy(j, q, q).wait_recv()
            value = value + arrived[j, q].astype(jnp.float32)
        grad[:, span] = value
        column = jnp.sum(value * value, axis=0, keepdims=True)
        for s in range(wc // 128):
            squares = squares + column[:, s * 128 : (s + 1) * 128]

    sq_all[me] = squares
    each_other_device(
        lambda to: remote(sq_all.at[me], sq_all.at[me], sq_send, sq_recv, to).start()
    )
    for load in states:
        load.wait()
    everyone = sq_all.at[pl.ds(0, total - 1)]
    pltpu.make_async_copy(everyone, everyone, sq_recv).wait()
    sumsq = jnp.sum(jnp.sum(sq_all[...], axis=0), axis=1, keepdims=True)
    rms = jnp.sqrt(sumsq / (rows * n * width * depth))
    factor = jnp.where(rms > 1.0, 1.0 / rms, 1.0)

    def cols(k):
        return pl.ds(k * wa, wa)

    def rows_of(d):
        return pl.ds(pl.multiple_of(d * rows, rows), rows)

    def gather_copy(k, d, to, send, recv):
        block = rows_out.at[rows_of(d), cols(k)]
        return remote(block, block, send, recv, to)

    def direct(k, source, q):
        return gather_copy(k, 2 * source + core, (2 * q + core, fs), ag_send.at[k, q], ag_recv.at[k, source])

    def relay(k, q, side):
        return gather_copy(k, 2 * q + side, partner, relay_send.at[k, q], relay_recv.at[k, q])

    for k in range(gathers):
        span = cols(k)
        clipped = factor * grad[:, span]
        new_one = 0.9 * one_v[:, span] + 0.1 * clipped
        new_two = 0.95 * two_v[:, span] + 0.05 * clipped * clipped
        first = new_one / (1.0 - 0.9**10)
        second = new_two / (1.0 - 0.95**10)
        held = mas_v[:, span]
        new_master = held - 0.05 * (first / (jnp.sqrt(second) + 1e-08) + 0.1 * held)
        rows_out[rows_of(dp), span] = new_master.astype(jnp.bfloat16)
        for q in others:
            direct(k, chip, q).start()
        relay(k, chip, core).start()
        one_out[:, span] = new_one
        two_out[:, span] = new_two
        mas_out[:, span] = new_master
    for k in range(gathers):
        for q in others:
            direct(k, q, q).wait_recv()
            relay(k, q, core).start()
    for k in range(gathers):
        for q in [chip] + others:
            relay(k, q, other).wait_recv()

    for j in range(chunks):
        pair_copy(j).wait_send()
        for q in others:
            chip_copy(j, q, chip).wait_send()
    pltpu.make_async_copy(everyone, everyone, sq_send).wait()
    for k in range(gathers):
        for q in others:
            direct(k, chip, q).wait_send()
            relay(k, q, core).wait_send()
        relay(k, chip, core).wait_send()


def spans(width, plan):
    unit, start, result = width // UNITS, 0, []
    for count, relayed in plan:
        result.append((start, count * unit, relayed))
        start += count * unit
    return result


def square_scratch(n, depth, tokens, slab, rows, width):
    f32, bf16 = jnp.float32, jnp.bfloat16
    dma = pltpu.SemaphoreType.DMA
    chunks = [(w, relayed) for _, w, relayed in spans(width, CHUNKS)]
    state = pltpu.VMEM((rows, width), f32)
    stage = tuple(pltpu.VMEM((2, n // 2, rows, w), bf16) for w, _ in chunks)
    paired = tuple(pltpu.VMEM((n // 2, rows, w), bf16) for w, _ in chunks)
    first = tuple(
        pltpu.VMEM((2, 2, rows, w // 2) if relayed else (3, rows, w), bf16) for w, relayed in chunks
    )
    second = tuple(pltpu.VMEM((2, rows, w // 2), bf16) for w, _ in chunks)
    many = len(chunks)
    return [
        pltpu.VMEM((tokens, slab), bf16),
        pltpu.VMEM((slab, tokens), bf16),
        tuple(pltpu.VMEM((tokens, w), bf16) for w, _ in chunks),
        state, state, state, state,
        stage, paired, first, first, second, second,
        tuple(pltpu.VMEM((4, 4, rows, width // UNITS), bf16) for _ in range(KITS)),
        pltpu.VMEM((n * depth, 1, 128), f32),
        dma((PARTS,)), dma((many,)), dma((3,)),
        dma, dma((many,)),
        dma((many,)), dma((many, 3)),
        dma((many,)), dma((many, 2)),
        dma, dma,
        dma((2,)), dma((len(PIECES), 3)),
        dma, dma((len(PIECES), 2)),
        dma, dma,
        dma((KITS,)), dma((KITS, 2, 3)),
    ]


def square_kernel(
    n, depth,
    hid, lgr, mas, one, two,
    rows_out, mas_out, one_out, two_out,
    lgr_v, lgt_v, hid_v, mas_v, one_v, two_v, grad,
    stage, paired, p1_out, p1_in, p2_out, p2_in, kit, sq_all,
    lgr_sem, hid_sem, state_sem, pair_send, pair_recv, p1_send, p1_recv, p2_send, p2_recv,
    sq_send, sq_recv, ag_send, ag_recv, far_send, far_recv, relay_send, relay_recv,
    kit_send, kit_recv,
):
    total = n * depth
    rows, width = grad.shape
    f32, bf16 = jnp.float32, jnp.bfloat16
    dp, fs = lax.axis_index("dp"), lax.axis_index("fsdp")
    chip, core = dp // 2, dp % 2
    other = 1 - core
    x, y = chip % 2, chip // 2
    near = (2 * y + 1 - x, 2 * (1 - y) + x)
    far = 2 * (1 - y) + 1 - x
    me = dp * depth + fs
    partner = (2 * chip + other, fs)
    across = tuple((2 * q + core, fs) for q in near + (far,))
    chunks, pieces_ = spans(width, CHUNKS), spans(width, PIECES)
    unit = width // UNITS
    kits = [width - (KITS - p) * unit for p in range(KITS)]
    steps = sorted(
        ((z, b, a, c) for z in range(depth) for b in range(2) for a in range(2) for c in range(2)),
        key=lambda s: -(min(s[0], depth - s[0]) + s[1] + s[2] + s[3] / 4),
    )[:-1]

    def each_other_device(act):
        for dz, b, a, c in steps:
            to_y = 1 - y if b else y
            to_x = 1 - x if a else x
            to_core = other if c else core
            act(((2 * to_y + to_x) * 2 + to_core, (fs + dz) % depth))

    def remote(src, dst, send, recv, to):
        return pltpu.make_async_remote_copy(
            src_ref=src, dst_ref=dst, send_sem=send, recv_sem=recv, device_id=to, device_id_type=MESH
        )

    def settle(ref, sem):
        pltpu.make_async_copy(ref, ref, sem).wait()

    step = lgr.shape[0] // PARTS
    lgr_loads = [
        pltpu.make_async_copy(lgr.at[pl.ds(i * step, step)], lgr_v.at[pl.ds(i * step, step)], lgr_sem.at[i])
        for i in range(PARTS)
    ]
    for load in lgr_loads:
        load.start()
    loads = [
        pltpu.make_async_copy(hid.at[:, pl.ds(start, w)], hid_v[j], hid_sem.at[j])
        for j, (start, w, _) in enumerate(chunks)
    ]
    loads[0].start(priority=1)
    barrier = pltpu.get_barrier_semaphore()
    each_other_device(
        lambda to: pl.semaphore_signal(barrier, inc=1, device_id=to, device_id_type=MESH)
    )
    states = [
        pltpu.make_async_copy(src, dst, state_sem.at[i])
        for i, (src, dst) in enumerate(((mas, mas_v), (one, one_v), (two, two_v)))
    ]

    def pair_copy(j):
        return remote(stage[j].at[other], paired[j], pair_send, pair_recv.at[j], partner)

    def first_copy(j, way):
        return remote(p1_out[j].at[way], p1_in[j].at[way], p1_send.at[j], p1_recv.at[j, way], across[way])

    def second_copy(j, way):
        return remote(p2_out[j].at[way], p2_in[j].at[way], p2_send.at[j], p2_recv.at[j, way], across[way])

    def both(j, q, start, w):
        cols = pl.ds(start, w)
        return stage[j][core, q, :, cols].astype(f32) + paired[j][q, :, cols].astype(f32)

    def chip_sum(j):
        start, w, relayed = chunks[j]
        wh = w // 2
        pair_copy(j).wait_recv()
        if relayed:
            for way in range(2):
                p1_out[j][way, 1] = both(j, far, way * wh, wh).astype(bf16)
                p1_out[j][way, 0] = both(j, near[way], way * wh, wh).astype(bf16)
                first_copy(j, way).start()
        else:
            for way, q in ((2, far), (0, near[0]), (1, near[1])):
                p1_out[j][way] = both(j, q, 0, w).astype(bf16)
                first_copy(j, way).start()
        grad[:, pl.ds(start, w)] = both(j, chip, 0, w)

    loads[1].start(priority=1)
    for i in range(PARTS):
        lgr_loads[i].wait()
        lgt_v[:, i * step : (i + 1) * step] = lgr_v[i * step : (i + 1) * step, :].T
    for load in loads[2:AHEAD]:
        load.start(priority=1)
    for j in range(len(chunks)):
        loads[j].wait()
        if j + AHEAD < len(chunks):
            loads[j + AHEAD].start(priority=1)
        elif j + AHEAD == len(chunks):
            for load in states:
                load.start()
        part = jnp.dot(lgt_v[...], hid_v[j][...], preferred_element_type=f32).astype(bf16)
        for q in range(n // 2):
            for c in range(2):
                d = 2 * q + c
                stage[j][c, q] = part[d * rows : (d + 1) * rows, :]
        if j == 0:
            pl.semaphore_wait(barrier, total - 1)
        pair_copy(j).start()
        if j > 0:
            chip_sum(j - 1)
    chip_sum(len(chunks) - 1)

    def state_copy(p, way):
        return remote(
            kit[p].at[3, pl.ds(0, 3)], kit[p].at[way, pl.ds(0, 3)], kit_send.at[p], kit_recv.at[p, 0, way], across[way]
        )

    def grad_copy(p, way):
        return remote(kit[p].at[3, 3], kit[p].at[way, 3], kit_send.at[p], kit_recv.at[p, 1, way], across[way])

    correct_one, correct_two = 1.0 - 0.9**10, 1.0 - 0.95**10
    for load in states:
        load.wait()
    for p, start in enumerate(kits):
        span = pl.ds(start, unit)
        held = mas_v[:, span]
        kit[p][3, 0] = (held - 0.05 * 0.1 * held).astype(bf16)
        kit[p][3, 1] = (0.05 * 0.9 / correct_one * one_v[:, span]).astype(bf16)
        kit[p][3, 2] = (0.95 / correct_two * two_v[:, span]).astype(bf16)
        if p < EARLY:
            for way in (2, 0, 1):
                state_copy(p, way).start()

    relayed_chunks = [j for j in range(len(chunks)) if chunks[j][2]]
    for j in relayed_chunks:
        wh = chunks[j][1] // 2
        for way in range(2):
            first_copy(j, way).wait_recv()
            away = 1 - way
            joined = both(j, near[away], way * wh, wh) + p1_in[j][way, 1].astype(f32)
            p2_out[j][away] = joined.astype(bf16)
            second_copy(j, away).start()

    squares = jnp.zeros((8, 128), f32)

    def add(start, w, terms, squares):
        span = pl.ds(start, w)
        value = grad[:, span]
        for term in terms:
            value = value + term.astype(f32)
        grad[:, span] = value
        value = value * value
        for r in range(rows // 8):
            for s in range(w // 128):
                squares = squares + value[r * 8 : (r + 1) * 8, s * 128 : (s + 1) * 128]
        return squares

    for j in relayed_chunks:
        start, w, _ = chunks[j]
        wh = w // 2
        for way in range(2):
            second_copy(j, 1 - way).wait_recv()
            squares = add(start + way * wh, wh, (p1_in[j][way, 0], p2_in[j][1 - way]), squares)
    for j, (start, w, relayed) in enumerate(chunks):
        if not relayed:
            for way in range(3):
                first_copy(j, way).wait_recv()
            squares = add(start, w, [p1_in[j][way] for way in range(3)], squares)

    sq_all[me] = jnp.sum(squares, axis=0, keepdims=True)
    def tell(to_y, to_x, to_core, to_z):
        to = ((2 * to_y + to_x) * 2 + to_core, to_z)
        remote(sq_all.at[me], sq_all.at[me], sq_send, sq_recv, to).start()

    for to_z in range(depth):
        for to_y, to_x, to_core in (
            (1 - y, 1 - x, other), (1 - y, 1 - x, core), (1 - y, x, other), (y, 1 - x, other),
            (1 - y, x, core), (y, 1 - x, core), (y, x, other),
        ):
            tell(to_y, to_x, to_core, to_z)
    for dz in range(1, depth):
        tell(y, x, core, (fs + dz) % depth)
    for p, start in enumerate(kits):
        kit[p][3, 3] = grad[:, pl.ds(start, unit)].astype(bf16)
        if p < EARLY:
            for way in (2, 0, 1):
                grad_copy(p, way).start()
    for p in range(EARLY, KITS):
        for way in (2, 0, 1):
            state_copy(p, way).start()
        for way in (2, 0, 1):
            grad_copy(p, way).start()
    everyone = sq_all.at[pl.ds(0, total - 1)]
    settle(everyone, sq_recv)
    sumsq = jnp.sum(jnp.sum(sq_all[...], axis=0), axis=1, keepdims=True)
    rms = jnp.sqrt(sumsq / (rows * n * width * depth))
    factor = jnp.where(rms > 1.0, 1.0 / rms, 1.0)

    def block(q, start, w):
        return rows_out.at[pl.ds(pl.multiple_of((2 * q + core) * rows, rows), rows), pl.ds(start, w)]

    def own_copy(k, way, q):
        start, w, relayed = pieces_[k]
        sem = ag_send.at[0 if relayed else 1]
        return remote(block(q, start, w), block(q, start, w), sem, ag_recv.at[k, way], across[way])

    def far_copy(k, way, q):
        start, w, _ = pieces_[k]
        part = block(q, start + way * (w // 2), w // 2)
        return remote(part, part, far_send, far_recv.at[k, way], across[1 - way])

    def relay(q, start, w):
        return remote(block(q, start, w), block(q, start, w), relay_send, relay_recv, partner)

    def update(start, w):
        span = pl.ds(start, w)
        clipped = factor * grad[:, span]
        new_one = 0.9 * one_v[:, span] + 0.1 * clipped
        new_two = 0.95 * two_v[:, span] + 0.05 * clipped * clipped
        first = new_one / correct_one
        second = new_two / correct_two
        held = mas_v[:, span]
        new_master = held - 0.05 * (first / (jnp.sqrt(second) + 1e-08) + 0.1 * held)
        one_out[:, span] = new_one
        two_out[:, span] = new_two
        mas_out[:, span] = new_master
        return new_master

    def rows_of(d):
        return pl.ds(pl.multiple_of(d * rows, rows), rows)

    for k, (start, w, relayed) in enumerate(pieces_):
        rows_out[rows_of(dp), pl.ds(start, w)] = update(start, w).astype(bf16)
        for way in (0, 1) if relayed else (2, 0, 1):
            own_copy(k, way, chip).start()
        relay(chip, start, w).start()
    for k, (start, w, relayed) in enumerate(pieces_):
        if relayed:
            for way in range(2):
                own_copy(k, way, near[way]).wait_recv()
                far_copy(k, way, near[way]).start()
                relay(near[way], start, w).start()
    for p, start in enumerate(kits):
        update(start, unit)
        for way in range(3):
            state_copy(p, way).wait_recv()
            grad_copy(p, way).wait_recv()
        for slot, q in enumerate(near + (far, chip)):
            base, step_one, step_two, part = (kit[p][slot, i].astype(f32) for i in range(4))
            clipped = factor * part
            step_one = step_one + 0.05 * 0.1 / correct_one * clipped
            step_two = step_two + 0.05 / correct_two * clipped * clipped
            new_rows = base - step_one / (jnp.sqrt(step_two) + 1e-08)
            rows_out[rows_of(2 * q + core), pl.ds(start, unit)] = new_rows.astype(bf16)
            relay(q, start, unit).start()

    for k, (start, w, relayed) in enumerate(pieces_):
        if not relayed:
            for way, q in ((0, near[0]), (1, near[1]), (2, far)):
                own_copy(k, way, q).wait_recv()
                relay(q, start, w).start()
    for k, (start, w, relayed) in enumerate(pieces_):
        if relayed:
            for way in range(2):
                far_copy(k, way, far).wait_recv()
                relay(far, start + way * (w // 2), w // 2).start()

    for j, (_, w, relayed) in enumerate(chunks):
        settle(paired[j], pair_send)
        settle(p1_in[j], p1_send.at[j])
        if relayed:
            settle(p2_in[j], p2_send.at[j])
    settle(everyone, sq_send)
    sent = sum(w for _, w, relayed in pieces_ if relayed)
    settle(rows_out.at[pl.ds(0, 2 * rows), pl.ds(0, sent)], ag_send.at[0])
    settle(rows_out.at[pl.ds(0, rows), pl.ds(0, sent)], far_send)
    straight = width - KITS * unit - sent
    if straight > 0:
        settle(rows_out.at[pl.ds(0, 3 * rows), pl.ds(0, straight)], ag_send.at[1])
    for p in range(KITS):
        settle(kit[p].at[pl.ds(0, 3)], kit_send.at[p])
    settle(rows_out.at[pl.ds(0, 4 * rows)], relay_send)
    settle(rows_out.at[pl.ds(0, 4 * rows)], relay_recv)


def write_out(*refs):
    sems = refs[8]
    copies = [pltpu.make_async_copy(refs[i], refs[4 + i], sems.at[i]) for i in range(4)]
    for copy in copies:
        copy.start()
    for copy in copies:
        copy.wait()


def shards(n, depth, hidden, logit_grad, master, moment_one, moment_two):
    tokens, width = hidden.shape
    slab = logit_grad.shape[1]
    rows = master.shape[0]
    chips = n // 2
    f32, bf16 = jnp.float32, jnp.bfloat16
    state = ((rows, width), f32)
    shapes = (((slab, width), bf16), state, state, state)
    kept = slab * width * 2 + 3 * rows * width * 4
    dma = pltpu.SemaphoreType.DMA
    anywhere = pl.BlockSpec(memory_space=pl.ANY)
    in_vmem = pl.BlockSpec(memory_space=pltpu.VMEM)
    if n == 8 and width % (UNITS * 256) == 0 and tokens % (PARTS * 128) == 0:
        body = functools.partial(square_kernel, n, depth)
        scratch = square_scratch(n, depth, tokens, slab, rows, width)
    else:
        chunks = pieces(width, LOAD_CHUNKS)
        gathers = pieces(width, GATHER_CHUNKS)
        wc = width // chunks
        body = functools.partial(direct_kernel, n, depth, chunks, gathers)
        scratch = [
            pltpu.VMEM((tokens, slab), bf16),
            pltpu.VMEM((slab, tokens), bf16),
            pltpu.VMEM((chunks, tokens, wc), bf16),
            pltpu.VMEM((rows, width), f32),
            pltpu.VMEM((rows, width), f32),
            pltpu.VMEM((rows, width), f32),
            pltpu.VMEM((chunks, 2, chips, rows, wc), bf16),
            pltpu.VMEM((chunks, chips, rows, wc), bf16),
            pltpu.VMEM((chunks, chips, rows, wc), bf16),
            pltpu.VMEM((chunks, chips, rows, wc), bf16),
            pltpu.VMEM((rows, width), f32),
            pltpu.VMEM((n * depth, 1, 128), f32),
            dma((chunks,)),
            dma,
            dma((3,)),
            dma((chunks,)),
            dma((chunks,)),
            dma((chunks, chips)),
            dma((chunks, chips)),
            dma,
            dma,
            dma((gathers, chips)),
            dma((gathers, chips)),
            dma((gathers, chips)),
            dma((gathers, chips)),
        ]
    held = pl.pallas_call(
        body,
        out_shape=tuple(pltpu.VMEM(*shape) for shape in shapes),
        in_specs=[anywhere] * 5,
        out_specs=(in_vmem,) * 4,
        scratch_shapes=scratch,
        compiler_params=pltpu.CompilerParams(
            collective_id=0, has_side_effects=True, vmem_limit_bytes=VMEM_BYTES - kept - 96 * 1024
        ),
    )(hidden, logit_grad, master, moment_one, moment_two)
    return pl.pallas_call(
        write_out,
        out_shape=tuple(pltpu.HBM(*shape) for shape in shapes),
        in_specs=[anywhere] * 4,
        out_specs=(anywhere,) * 4,
        scratch_shapes=[dma((4,))],
        compiler_params=pltpu.CompilerParams(vmem_limit_bytes=1024 * 1024),
    )(*held)


def solution(mesh):
    placed = (P("dp", "fsdp"), P("dp", None), P("dp", "fsdp"), P("dp", "fsdp"), P("dp", "fsdp"))
    return jax.shard_map(
        functools.partial(shards, mesh.shape["dp"], mesh.shape["fsdp"]),
        mesh=mesh,
        in_specs=placed,
        out_specs=(P(None, "fsdp"), P("dp", "fsdp"), P("dp", "fsdp"), P("dp", "fsdp")),
        check_vma=False,
    )
```
